32 devices in a mesh: tp: 2 (over x), cp: 16 (over z, y, core).
Axes of the slice: x: 2, y: 2, z: 4, core: 2. Of those that a mesh axis runs over, the one named last changes fastest.
Arguments:
- q_raw: bfloat16 [4096, 32, 128], P('cp', 'tp'), parts along dimension 1
- k_raw: bfloat16 [4096, 8, 128], P('cp', 'tp'), parts along dimension 1
- v_raw: bfloat16 [4096, 8, 128], P('cp', 'tp'), parts along dimension 1
- positions: int32 [4096], P('cp')
- seq_ids: int32 [4096], P('cp')
- q_gain: bfloat16 [128], replicated
- k_gain: bfloat16 [128], replicated
Outputs:
- output 1: bfloat16 [4096, 32, 128], P('cp', 'tp'), parts along dimension 1
- output 2: float32 [4096, 32], P('cp', 'tp'), parts along dimension 1
There are 2 independent parts. The reference program is written for one: setup_inputs(seed, part) draws one part's arguments, and reference() takes and returns one part's arrays. A program takes and returns all parts, laid end to end along the dimension named above; an argument that names none is the same for every part.
All inputs are finite; a program needn't handle non-finite values.
Results may differ from the reference program's by a relative error of at most 0.013793.
Values are sent between devices in bfloat16 or wider.
A program may use at most 1 GiB of HBM per device.

```python
import jax
import jax.numpy as jnp
from jax import lax

N_TOKENS = 4096
PART_Q_HEADS = 16
PART_KV_HEADS = 4
HEAD_DIM = 128
CP_SIZE = 16
SEQ_COUNT = 4
ROW_BLOCK = 64
THETA = 1000000.0
EPS = 1e-6
NEG_BIG = -1e30


def draw_layout(key):
    units = N_TOKENS // (2 * CP_SIZE)
    picks = jax.random.permutation(key, units - 1)[: SEQ_COUNT - 1] + 1
    cuts = jnp.sort(picks).astype(jnp.int32)
    bounds = jnp.concatenate([jnp.zeros((1,), jnp.int32), cuts, jnp.full((1,), units, jnp.int32)])
    lengths = bounds[1:] - bounds[:-1]
    local_idx = jnp.arange(2 * units, dtype=jnp.int32)
    seq_local = jnp.sum((local_idx[:, None] >= 2 * cuts[None, :]).astype(jnp.int32), axis=1)
    piece_len = lengths[seq_local]
    within = local_idx - 2 * bounds[seq_local]
    first_half = within < piece_len
    device_idx = jnp.arange(CP_SIZE, dtype=jnp.int32)[:, None]
    piece_idx = jnp.where(first_half[None, :], device_idx, 2 * CP_SIZE - 1 - device_idx)
    offset = jnp.where(first_half, within, within - piece_len)
    positions = piece_idx * piece_len[None, :] + offset[None, :]
    seq_ids = jnp.broadcast_to(seq_local[None, :], (CP_SIZE, 2 * units))
    return positions.reshape(N_TOKENS).astype(jnp.int32), seq_ids.reshape(N_TOKENS).astype(jnp.int32)


def setup_inputs(seed: int = 0, part: int = 0) -> dict:
    key = jax.random.key(seed)
    key_layout, key_gq, key_gk, key_vals = jax.random.split(key, 4)
    positions, seq_ids = draw_layout(key_layout)
    part_key = jax.random.fold_in(key_vals, part)
    key_q, key_k, key_v = jax.random.split(part_key, 3)
    q_raw = jax.random.normal(key_q, (N_TOKENS, PART_Q_HEADS, HEAD_DIM), jnp.float32).astype(jnp.bfloat16)
    k_raw = jax.random.normal(key_k, (N_TOKENS, PART_KV_HEADS, HEAD_DIM), jnp.float32).astype(jnp.bfloat16)
    v_raw = jax.random.normal(key_v, (N_TOKENS, PART_KV_HEADS, HEAD_DIM), jnp.float32).astype(jnp.bfloat16)
    q_gain = (1.3 + 0.4 * jax.random.normal(key_gq, (HEAD_DIM,), jnp.float32)).astype(jnp.bfloat16)
    k_gain = (1.3 + 0.4 * jax.random.normal(key_gk, (HEAD_DIM,), jnp.float32)).astype(jnp.bfloat16)
    return {"q_raw": q_raw, "k_raw": k_raw, "v_raw": v_raw, "positions": positions, "seq_ids": seq_ids, "q_gain": q_gain, "k_gain": k_gain}


def norm_rope(x_in, gain, positions):
    head_dim = x_in.shape[-1]
    half = head_dim // 2
    x_f32 = x_in.astype(jnp.float32)
    inv_rms = lax.rsqrt(jnp.mean(x_f32 * x_f32, axis=-1, keepdims=True) + EPS)
    normed = (x_f32 * inv_rms * gain.astype(jnp.float32)).astype(jnp.bfloat16).astype(jnp.float32)
    inv_freq = jnp.power(THETA, -(jnp.arange(half, dtype=jnp.float32) * 2.0) / head_dim)
    angle = positions.astype(jnp.float32)[:, None] * inv_freq[None, :]
    cos_a = jnp.cos(angle)[:, None, :]
    sin_a = jnp.sin(angle)[:, None, :]
    first = normed[..., :half]
    second = normed[..., half:]
    rotated = jnp.concatenate([first * cos_a - second * sin_a, second * cos_a + first * sin_a], axis=-1)
    return rotated.astype(jnp.bfloat16)


def reference(q_raw, k_raw, v_raw, positions, seq_ids, q_gain, k_gain):
    group = PART_Q_HEADS // PART_KV_HEADS
    scale = HEAD_DIM ** -0.5
    q_rot = norm_rope(q_raw, q_gain, positions)
    k_all = norm_rope(k_raw, k_gain, positions).astype(jnp.float32)
    v_all = v_raw.astype(jnp.float32)
    n_blocks = N_TOKENS // ROW_BLOCK
    q_blocks = q_rot.reshape(n_blocks, ROW_BLOCK, PART_KV_HEADS, group, HEAD_DIM)
    pos_blocks = positions.reshape(n_blocks, ROW_BLOCK)
    seq_blocks = seq_ids.reshape(n_blocks, ROW_BLOCK)

    def one_block(block_in):
        q_blk, q_pos, q_seq = block_in
        scores = jnp.einsum("rkgd,skd->rkgs", q_blk.astype(jnp.float32), k_all) * scale
        allowed = (q_seq[:, None] == seq_ids[None, :]) & (positions[None, :] <= q_pos[:, None])
        scores = jnp.where(allowed[:, None, None, :], scores, NEG_BIG)
        row_max = jnp.max(scores, axis=-1)
        weights = jnp.exp(scores - row_max[..., None])
        row_sum = jnp.sum(weights, axis=-1)
        attn_blk = jnp.einsum("rkgs,skd->rkgd", weights, v_all) / row_sum[..., None]
        log_sum = row_max + jnp.log(row_sum)
        return attn_blk.astype(jnp.bfloat16).reshape(ROW_BLOCK, PART_Q_HEADS, HEAD_DIM), log_sum.reshape(ROW_BLOCK, PART_Q_HEADS)

    attn_blocks, log_blocks = lax.map(one_block, (q_blocks, pos_blocks, seq_blocks))
    return attn_blocks.reshape(N_TOKENS, PART_Q_HEADS, HEAD_DIM), log_blocks.reshape(N_TOKENS, PART_Q_HEADS)
```

```python
import functools
import math

import jax
import jax.numpy as jnp
import numpy as np
from jax import lax
from jax.experimental import pallas as pl
from jax.experimental.pallas import tpu as pltpu
from jax.sharding import PartitionSpec as P

THETA = 1000000.0
EPS = 1e-6
NEG = -1e30
LAYERS = 4
CHIPS = 8
CP = 16
T = 256
HALF = 128
KVH = 4
GROUP = 4
QH = KVH * GROUP
D = 128
RC = 256
LOG2E = math.log2(math.e)
LN2 = math.log(2.0)
SCALE2 = D ** -0.5 * LOG2E
ORDER = ((1, 2, 3), (0, 2, 3), (1, 3, 0), (2, 1, 0))
TABLE = sum(ORDER[z][k] << (2 * (3 * z + k)) for z in range(LAYERS) for k in range(3))

E, L = 0, 1
F32 = jnp.float32
BF16 = jnp.bfloat16
MESH = pl.DeviceIdType.MESH


def dot(a, b, dims, precision=None):
    return lax.dot_general(a, b, (dims, ((), ())), preferred_element_type=F32, precision=precision)


def column(row, ident):
    return jnp.sum(jnp.where(ident, row, 0.0), axis=1, keepdims=True)


def norm_rope(x, gain, cos, sin):
    inv = lax.rsqrt(jnp.mean(x * x, axis=-1, keepdims=True) + EPS)
    normed = (x * inv * gain).astype(BF16).astype(F32)
    return (normed * cos + pltpu.roll(normed, D // 2, 1) * sin).astype(BF16)


def kernel(q_ref, k_ref, v_ref, pos_ref, seq_ref, qg_ref, kg_ref, freq_ref, o_ref, lse_ref,
           kvbuf, qbuf, acc, mst, lst, bias, rope, perm,
           s_dn, s_up, s_y, s_d, r_link, r_d):
    me = lax.axis_index("cp")
    z = me // 4
    y = (me // 2) % 2
    c = me % 2
    own = me // 2

    def dev(zz, yy, cc):
        return {"cp": zz * 4 + yy * 2 + cc}

    barrier = pltpu.get_barrier_semaphore()
    pl.semaphore_signal(barrier, inc=1, device_id=dev(z, y, 1 - c), device_id_type=MESH)
    pl.semaphore_signal(barrier, inc=1, device_id=dev(z, 1 - y, c), device_id_type=MESH)

    @pl.when(z > 0)
    def _():
        pl.semaphore_signal(barrier, inc=1, device_id=dev(z - 1, y, c), device_id_type=MESH)

    @pl.when(z < LAYERS - 1)
    def _():
        pl.semaphore_signal(barrier, inc=1, device_id=dev(z + 1, y, c), device_id_type=MESH)

    row_i = lax.broadcasted_iota(jnp.int32, (T, T), 0)
    col_i = lax.broadcasted_iota(jnp.int32, (T, T), 1)
    ident = row_i == col_i
    pos_row = pos_ref[...].astype(F32)
    seq_row = seq_ref[...].astype(F32)
    pos_col = column(pos_row, ident)
    seq_col = column(seq_row, ident)
    same = (seq_col == seq_row).astype(F32)
    early_row = (pos_row < 8.0 * jnp.sum(same, axis=0, keepdims=True)).astype(F32)
    early_col = (pos_col < 8.0 * jnp.sum(same, axis=1, keepdims=True)).astype(F32)
    alike = (early_col == early_row).astype(F32)
    dest_row = jnp.sum(jnp.where(row_i < col_i, alike, 0.0), axis=0, keepdims=True) + HALF * (1.0 - early_row)
    one_hot = (row_i.astype(F32) == dest_row).astype(BF16)
    perm[...] = one_hot

    angle = pos_col * freq_ref[...]
    cos = jnp.cos(angle)
    sin = jnp.sin(angle)
    sin = jnp.where(lax.broadcasted_iota(jnp.int32, (T, D), 1) < D // 2, -sin, sin)
    rope[0] = cos
    rope[1] = sin

    k_all = jnp.transpose(k_ref[...].astype(F32), (1, 0, 2))
    v_all = jnp.transpose(v_ref[...].astype(F32), (1, 0, 2)).astype(BF16)
    gain = kg_ref[...].astype(F32)
    for h in range(KVH):
        kr = dot(one_hot, norm_rope(k_all[h], gain, cos, sin), ((1,), (0,))).astype(BF16)
        vr = dot(one_hot, v_all[h], ((1,), (0,))).astype(BF16)
        for part in (E, L):
            kvbuf[own, part, 0, h, c] = kr[part * HALF:(part + 1) * HALF]
            kvbuf[own, part, 1, h, c] = vr[part * HALF:(part + 1) * HALF]

    pl.semaphore_wait(barrier, 2 + jnp.minimum(z, 1) + jnp.minimum(LAYERS - 1 - z, 1))

    def copy(m, part, lane, send, recv, target):
        ref = kvbuf.at[m, part, :, :, lane]
        return pltpu.make_async_remote_copy(
            src_ref=ref, dst_ref=ref, send_sem=send.at[m, part], recv_sem=recv.at[m, part],
            device_id=target, device_id_type=MESH)

    def down(m, part):
        return copy(m, part, c, s_dn, r_link, dev(z - 1, y, c))

    def up(m, part):
        return copy(m, part, c, s_up, r_link, dev(z + 1, y, c))

    def across(m, part):
        return copy(m, part, c, s_y, r_link, dev(z, 1 - y, c))

    def partner(m, part):
        return copy(m, part, c, s_d, r_d, dev(z, y, 1 - c))

    def sends(m):
        mz = m // 2
        my = m % 2
        corner = jnp.logical_and(m == CHIPS - 1, y == 0)
        above = mz >= z
        below = mz <= z
        e_down = jnp.logical_and(z > 0, jnp.logical_and(above, jnp.logical_or(my == y, corner)))
        e_up = jnp.logical_and(z < LAYERS - 1, jnp.logical_and(below, my == y))
        skip = jnp.logical_and(m == CHIPS - 1, z < LAYERS - 1)
        e_across = jnp.logical_and(my == y, jnp.logical_not(skip))
        l_down = jnp.logical_and(z > 0, jnp.logical_and(above, my == y))
        l_across = jnp.logical_and(my == y, m > z * 2 + 1 - y)
        return e_down, e_up, e_across, l_down, l_across

    def forward_early(m):
        e_down, e_up, e_across, _, _ = sends(m)

        @pl.when(e_down)
        def _():
            down(m, E).start()

        @pl.when(e_across)
        def _():
            across(m, E).start()

        @pl.when(e_up)
        def _():
            up(m, E).start()

        partner(m, E).start()

    def forward_late(m):
        _, _, _, l_down, l_across = sends(m)

        @pl.when(l_down)
        def _():
            down(m, L).start()

        @pl.when(l_across)
        def _():
            across(m, L).start()

        partner(m, L).start()

    forward_early(own)
    forward_late(own)

    q_all = jnp.transpose(q_ref[...].astype(F32), (1, 0, 2))
    q_gain = qg_ref[...].astype(F32)
    for h in range(QH):
        qr = dot(perm[...], norm_rope(q_all[h], q_gain, rope[0], rope[1]), ((1,), (0,))).astype(BF16)
        for part in (E, L):
            qbuf[part, h // GROUP, (h % GROUP) * HALF:(h % GROUP + 1) * HALF] = qr[part * HALF:(part + 1) * HALF]

    seg = dot(perm[0:HALF], same.astype(BF16), ((1,), (0,))).astype(BF16)
    seg = dot(seg, perm[0:HALF], ((1,), (1,))) > 0.5
    r_i = lax.broadcasted_iota(jnp.int32, (HALF, HALF), 0)
    c_i = lax.broadcasted_iota(jnp.int32, (HALF, HALF), 1)
    full = jnp.where(seg, 0.0, NEG)
    diag = jnp.where(jnp.logical_and(seg, c_i <= r_i), 0.0, NEG)
    none = jnp.full((HALF, HALF), NEG, F32)
    first = c == 0
    e_left, e_right = jnp.where(first, diag, full), jnp.where(first, none, diag)
    l_left, l_right = jnp.where(first, diag, none), jnp.where(first, full, diag)
    for i in range(RC // HALF):
        rows = slice(i * HALF, (i + 1) * HALF)
        bias[0, rows, 0:HALF] = full
        bias[0, rows, HALF:] = full
        bias[1, rows, 0:HALF] = e_left
        bias[1, rows, HALF:] = e_right
        bias[2, rows, 0:HALF] = l_left
        bias[2, rows, HALF:] = l_right

    mst[...] = jnp.full(mst.shape, NEG, F32)
    lst[...] = jnp.zeros(lst.shape, F32)
    acc[...] = jnp.zeros(acc.shape, F32)

    def attend(qp, h, r, m, parts):
        rows = pl.ds(r * RC, RC)
        q = qbuf[qp, h, rows]
        scores = []
        for part, b in parts:
            keys = kvbuf[m, part, 0, h].reshape(2 * HALF, D)
            scores.append(dot(q, keys, ((1,), (1,))) * SCALE2 + bias[b])
        top = scores[0]
        for s in scores[1:]:
            top = jnp.maximum(top, s)
        m_old = mst[qp, h, rows]
        m_new = jnp.maximum(m_old, jnp.max(top, axis=1, keepdims=True))
        alpha = jnp.exp2(m_old - m_new)
        m_wide = jnp.concatenate([m_new, m_new], axis=1)
        l_new = lst[qp, h, rows] * alpha
        out = acc[qp, h, rows] * alpha
        for (part, _), s in zip(parts, scores):
            p = jnp.exp2(s - m_wide)
            l_new = l_new + p[:, 0:HALF] + p[:, HALF:]
            vals = kvbuf[m, part, 1, h].reshape(2 * HALF, D)
            out = out + dot(p.astype(BF16), vals, ((1,), (0,)))
        mst[qp, h, rows] = m_new
        lst[qp, h, rows] = l_new
        acc[qp, h, rows] = out

    chunks = GROUP * HALF // RC

    partner(own, E).wait_recv()
    partner(own, L).wait_recv()

    @pl.loop(0, KVH)
    def _(h):
        for r in range(chunks):
            attend(E, h, r, own, [(E, 1)])
            attend(L, h, r, own, [(L, 2), (E, 0)])

    @pl.loop(0, CHIPS - 1)
    def _(n):
        k = (n + 1) // 2
        other = lax.rem(jnp.right_shift(TABLE, 2 * (3 * z + jnp.maximum(k - 1, 0))), 4)
        mz = jnp.where(n == 0, z, other)
        my = jnp.where(n % 2 == 0, 1 - y, y)
        m = mz * 2 + my

        across(m, E).wait_recv()
        forward_early(m)

        @pl.when(m > own)
        def _():
            across(m, L).wait_recv()
            forward_late(m)

        partner(m, E).wait_recv()

        @pl.when(m > own)
        def _():
            partner(m, L).wait_recv()

            @pl.loop(0, KVH)
            def _(h):
                for r in range(chunks):
                    attend(L, h, r, m, [(E, 0), (L, 0)])

        @pl.when(m < own)
        def _():
            @pl.loop(0, KVH)
            def _(h):
                for r in range(chunks):
                    attend(E, h, r, m, [(E, 0)])
                    attend(L, h, r, m, [(E, 0)])

    lane = lax.broadcasted_iota(jnp.int32, (T, D), 1)
    lse = jnp.zeros((T, D), F32)
    for h in range(KVH):
        outs = []
        logs = []
        for part in (E, L):
            total = jnp.sum(lst[part, h], axis=1, keepdims=True)
            outs.append((acc[part, h] / total).astype(BF16))
            logs.append(mst[part, h] * LN2 + jnp.log(total))
        for g in range(GROUP):
            rows = slice(g * HALF, (g + 1) * HALF)
            both = jnp.concatenate([outs[0][rows], outs[1][rows]], axis=0)
            o_ref[h * GROUP + g] = dot(perm[...], both, ((0,), (0,))).astype(BF16)
            both = jnp.concatenate([logs[0][rows], logs[1][rows]], axis=0)
            lse = jnp.where(lane == h * GROUP + g, both, lse)
    lse = dot(perm[...].astype(F32), lse, ((0,), (0,)), precision=lax.Precision.HIGHEST)
    lse_ref[...] = lse[:, 0:QH]

    @pl.loop(0, CHIPS)
    def _(m):
        e_down, e_up, e_across, l_down, l_across = sends(m)

        @pl.when(e_down)
        def _():
            down(m, E).wait_send()

        @pl.when(e_across)
        def _():
            across(m, E).wait_send()

        @pl.when(e_up)
        def _():
            up(m, E).wait_send()

        partner(m, E).wait_send()

        @pl.when(m >= own)
        def _():
            partner(m, L).wait_send()

        @pl.when(jnp.logical_and(m >= own, l_down))
        def _():
            down(m, L).wait_send()

        @pl.when(jnp.logical_and(m >= own, l_across))
        def _():
            across(m, L).wait_send()


def solution(mesh):
    half = np.arange(D // 2, dtype=np.float32) * np.float32(2.0) / np.float32(D)
    freq = np.power(np.float64(THETA), -half.astype(np.float64)).astype(np.float32)
    freq = np.concatenate([freq, freq])[None, :]

    def per_device(q_raw, k_raw, v_raw, positions, seq_ids, q_gain, k_gain):
        vmem = pl.BlockSpec(memory_space=pltpu.VMEM)
        sem = pltpu.SemaphoreType.DMA((CHIPS, 2))
        out, lse = pl.pallas_call(
            kernel,
            out_shape=(jax.ShapeDtypeStruct((QH, T, D), BF16), jax.ShapeDtypeStruct((T, QH), F32)),
            in_specs=[vmem] * 8,
            out_specs=(vmem, vmem),
            scratch_shapes=[
                pltpu.VMEM((CHIPS, 2, 2, KVH, 2, HALF, D), BF16),
                pltpu.VMEM((2, KVH, GROUP * HALF, D), BF16),
                pltpu.VMEM((2, KVH, GROUP * HALF, D), F32),
                pltpu.VMEM((2, KVH, GROUP * HALF, D), F32),
                pltpu.VMEM((2, KVH, GROUP * HALF, D), F32),
                pltpu.VMEM((3, RC, 2 * HALF), F32),
                pltpu.VMEM((2, T, D), F32),
                pltpu.VMEM((T, T), BF16),
                sem, sem, sem, sem, sem, sem,
            ],
            compiler_params=pltpu.CompilerParams(collective_id=0, has_side_effects=True, vmem_limit_bytes=48 * 1024 * 1024),
            name="gather_attend",
        )(q_raw, k_raw, v_raw, positions[None, :], seq_ids[None, :], q_gain[None, :], k_gain[None, :], jnp.asarray(freq))
        return jnp.transpose(out, (1, 0, 2)), lse

    return jax.shard_map(per_device, mesh=mesh, in_specs=(P("cp", "tp", None), P("cp", "tp", None), P("cp", "tp", None), P("cp"), P("cp"), P(), P()), out_specs=(P("cp", "tp", None), P("cp", "tp")), check_vma=False)
```

```python
import functools
import math

import jax
import jax.numpy as jnp
import numpy as np
from jax import lax
from jax.experimental import pallas as pl
from jax.experimental.pallas import tpu as pltpu
from jax.sharding import PartitionSpec as P

THETA = 1000000.0
EPS = 1e-6
NEG = -1e30
LAYERS = 4
CHIPS = 8
CP = 16
T = 256
HALF = 128
KVH = 4
GROUP = 4
QH = KVH * GROUP
D = 128
LOG2E = math.log2(math.e)
LN2 = math.log(2.0)
SCALE2 = D ** -0.5 * LOG2E
EVENTS = (
    (32, 4, 8, 33, 5, 9, 6, 10, 7, 11, 36, 37, 12, 16, 40, 41, 13, 17, 14, 18, 15, 19, 44, 45, 20, 24, 48, 49, 21, 25, 22, 26, 23, 27, 52, 53, 28, 30, 56, 57, 29, 31, 60, 61),
    (36, 0, 12, 37, 1, 13, 32, 33, 8, 14, 9, 15, 44, 45, 20, 10, 21, 11, 40, 41, 16, 22, 17, 23, 52, 53, 28, 18, 29, 19, 48, 49, 24, 30, 25, 31, 60, 61, 26, 27, 56, 57),
    (40, 0, 12, 16, 41, 1, 13, 17, 32, 33, 14, 18, 15, 19, 44, 45, 4, 24, 48, 49, 20, 25, 5, 26, 36, 37, 21, 27, 56, 28, 22, 57, 29, 23, 52, 53, 30, 31, 60, 61),
    (44, 4, 8, 20, 45, 5, 9, 21, 36, 37, 0, 22, 40, 41, 16, 23, 52, 28, 1, 53, 32, 17, 29, 33, 18, 30, 19, 31, 48, 49, 24, 60, 61, 25, 26, 27, 56, 57),
    (48, 8, 20, 24, 49, 9, 21, 25, 40, 41, 0, 22, 26, 1, 23, 27, 32, 33, 12, 28, 52, 53, 13, 29, 56, 57, 4, 44, 45, 30, 5, 36, 37, 31, 60, 61),
    (52, 12, 16, 28, 53, 13, 17, 29, 44, 45, 4, 8, 30, 48, 49, 24, 5, 31, 36, 9, 37, 40, 25, 41, 60, 0, 61, 26, 1, 32, 33, 27, 56, 57),
    (56, 16, 28, 57, 17, 29, 48, 49, 8, 30, 9, 31, 40, 41, 0, 20, 60, 61, 1, 21, 32, 12, 33, 52, 13, 53, 44, 4, 45, 5, 36, 37),
    (60, 20, 24, 61, 21, 25, 52, 53, 12, 16, 56, 57, 13, 17, 44, 4, 8, 45, 48, 9, 5, 49, 36, 0, 37, 40, 1, 41, 32, 33),
)
NOTHING = 64
STEPS = max(len(e) for e in EVENTS)
BITS = 7
PER_WORD = 4
WORDS = -(-STEPS // PER_WORD)
PARTS = 4


def packed(chip, word):
    events = EVENTS[chip] + (NOTHING,) * (WORDS * PER_WORD)
    return sum(events[word * PER_WORD + i] << (BITS * i) for i in range(PER_WORD))


E, L = 0, 1
F32 = jnp.float32
BF16 = jnp.bfloat16
MESH = pl.DeviceIdType.MESH


def dot(a, b, dims, precision=None):
    return lax.dot_general(a, b, (dims, ((), ())), preferred_element_type=F32, precision=precision)


def column(row, ident):
    return jnp.sum(jnp.where(ident, row, 0.0), axis=1, keepdims=True)


def norm_rope(x, gain, cos, sin):
    inv = lax.rsqrt(jnp.mean(x * x, axis=-1, keepdims=True) + EPS)
    normed = (x * inv * gain).astype(BF16).astype(F32)
    return (normed * cos + pltpu.roll(normed, D // 2, 1) * sin).astype(BF16)


def kernel(q_ref, k_ref, v_ref, pos_ref, seq_ref, qg_ref, kg_ref, freq_ref, o_ref, lse_ref,
           kvbuf, qbuf, acc, mst, lst, bias, rope, perm,
           s_dn, s_up, s_y, s_d, r_link, r_d):
    me = lax.axis_index("cp")
    z = me // 4
    y = (me // 2) % 2
    c = me % 2
    own = me // 2

    def dev(zz, yy, cc):
        return {"cp": zz * 4 + yy * 2 + cc}

    barrier = pltpu.get_barrier_semaphore()
    pl.semaphore_signal(barrier, inc=1, device_id=dev(z, y, 1 - c), device_id_type=MESH)
    pl.semaphore_signal(barrier, inc=1, device_id=dev(z, 1 - y, c), device_id_type=MESH)

    @pl.when(z > 0)
    def _():
        pl.semaphore_signal(barrier, inc=1, device_id=dev(z - 1, y, c), device_id_type=MESH)

    @pl.when(z < LAYERS - 1)
    def _():
        pl.semaphore_signal(barrier, inc=1, device_id=dev(z + 1, y, c), device_id_type=MESH)

    row_i = lax.broadcasted_iota(jnp.int32, (T, T), 0)
    col_i = lax.broadcasted_iota(jnp.int32, (T, T), 1)
    ident = row_i == col_i
    pos_row = pos_ref[...].astype(F32)
    seq_row = seq_ref[...].astype(F32)
    pos_col = column(pos_row, ident)
    seq_col = column(seq_row, ident)
    same = (seq_col == seq_row).astype(F32)
    early_row = (pos_row < 8.0 * jnp.sum(same, axis=0, keepdims=True)).astype(F32)
    early_col = (pos_col < 8.0 * jnp.sum(same, axis=1, keepdims=True)).astype(F32)
    alike = (early_col == early_row).astype(F32)
    dest_row = jnp.sum(jnp.where(row_i < col_i, alike, 0.0), axis=0, keepdims=True) + HALF * (1.0 - early_row)
    one_hot = (row_i.astype(F32) == dest_row).astype(BF16)
    perm[...] = one_hot

    angle = pos_col * freq_ref[...]
    cos = jnp.cos(angle)
    sin = jnp.sin(angle)
    sin = jnp.where(lax.broadcasted_iota(jnp.int32, (T, D), 1) < D // 2, -sin, sin)
    rope[0] = cos
    rope[1] = sin

    k_all = jnp.transpose(k_ref[...].astype(F32), (1, 0, 2))
    v_all = jnp.transpose(v_ref[...].astype(F32), (1, 0, 2)).astype(BF16)
    gain = kg_ref[...].astype(F32)
    for h in range(KVH):
        kr = dot(one_hot, norm_rope(k_all[h], gain, cos, sin), ((1,), (0,))).astype(BF16)
        vr = dot(v_all[h], one_hot, ((0,), (1,))).astype(BF16)
        for part in (E, L):
            kvbuf[own, 2 * part, h, c] = kr[part * HALF:(part + 1) * HALF]
            kvbuf[own, 2 * part + 1, h, c] = vr[:, part * HALF:(part + 1) * HALF]

    pl.semaphore_wait(barrier, 2 + jnp.minimum(z, 1) + jnp.minimum(LAYERS - 1 - z, 1))

    def copy(m, part, send, recv, target):
        ref = kvbuf.at[m, part, :, c]
        return pltpu.make_async_remote_copy(
            src_ref=ref, dst_ref=ref, send_sem=send.at[m, part], recv_sem=recv.at[m, part],
            device_id=target, device_id_type=MESH)

    def down(m, part):
        return copy(m, part, s_dn, r_link, dev(z - 1, y, c))

    def up(m, part):
        return copy(m, part, s_up, r_link, dev(z + 1, y, c))

    def across(m, part):
        return copy(m, part, s_y, r_link, dev(z, 1 - y, c))

    def partner(m, part):
        return copy(m, part, s_d, r_d, dev(z, y, 1 - c))

    def routes(m, part):
        mz = m // 2
        straight = m % 2 == y
        early = part < 2
        both = jnp.logical_and(early, m == CHIPS - 1)
        go_down = (z > 0) & (mz >= z) & (straight | (both & (y == 0)))
        go_across = straight & jnp.where(early, ~(both & (z < LAYERS - 1)), m > z * 2 + 1 - y)
        go_up = early & (z < LAYERS - 1) & (mz <= z) & straight
        return go_down, go_across, go_up

    def forward(m, part):
        go_down, go_across, go_up = routes(m, part)

        @pl.when(go_down)
        def _():
            down(m, part).start()

        @pl.when(go_across)
        def _():
            across(m, part).start()

        @pl.when(go_up)
        def _():
            up(m, part).start()

        partner(m, part).start()

    @pl.loop(0, PARTS)
    def _(part):
        forward(own, part)

    q_all = jnp.transpose(q_ref[...].astype(F32), (1, 0, 2))
    q_gain = qg_ref[...].astype(F32)
    for h in range(QH):
        qr = dot(norm_rope(q_all[h], q_gain, rope[0], rope[1]), perm[...], ((0,), (1,))).astype(BF16)
        for part in (E, L):
            qbuf[part, h // GROUP, :, (h % GROUP) * HALF:(h % GROUP + 1) * HALF] = qr[:, part * HALF:(part + 1) * HALF]

    seg = dot(perm[0:HALF], same.astype(BF16), ((1,), (0,))).astype(BF16)
    seg = dot(seg, perm[0:HALF], ((1,), (1,))) > 0.5
    r_i = lax.broadcasted_iota(jnp.int32, (HALF, HALF), 0)
    c_i = lax.broadcasted_iota(jnp.int32, (HALF, HALF), 1)
    full = jnp.where(seg, 0.0, NEG)
    diag = jnp.where(jnp.logical_and(seg, r_i <= c_i), 0.0, NEG)
    none = jnp.full((HALF, HALF), NEG, F32)
    first = c == 0
    bias[0, 0:HALF] = full
    bias[0, HALF:] = full
    bias[1, 0:HALF] = jnp.where(first, diag, full)
    bias[1, HALF:] = jnp.where(first, none, diag)
    bias[2, 0:HALF] = jnp.where(first, diag, none)
    bias[2, HALF:] = jnp.where(first, full, diag)

    mst[...] = jnp.full(mst.shape, NEG, F32)
    lst[...] = jnp.zeros(lst.shape, F32)
    acc[...] = jnp.zeros(acc.shape, F32)

    def attend(qp, h, m, parts):
        q = qbuf[qp, h]
        scores = []
        for part, b in parts:
            keys = kvbuf[m, 2 * part, h].reshape(2 * HALF, D)
            wide = jnp.concatenate([bias[b]] * GROUP, axis=1)
            scores.append(dot(keys, q, ((1,), (0,))) * SCALE2 + wide)
        m_old = mst[qp, h]
        m_new = m_old
        for s in scores:
            m_new = jnp.maximum(m_new, jnp.max(s, axis=0, keepdims=True))
        alpha = jnp.exp2(m_old - m_new)
        l_new = lst[qp, h] * alpha
        out = acc[qp, h] * alpha
        for (part, _), s in zip(parts, scores):
            p = jnp.exp2(s - m_new)
            l_new = l_new + jnp.sum(p, axis=0, keepdims=True)
            vals = jnp.concatenate([kvbuf[m, 2 * part + 1, h, 0], kvbuf[m, 2 * part + 1, h, 1]], axis=1)
            out = out + dot(vals, p.astype(BF16), ((1,), (0,)))
        mst[qp, h] = m_new
        lst[qp, h] = l_new
        acc[qp, h] = out

    def arrived(m, parts):
        for part in parts:
            partner(m, part).wait_recv()

    words = []
    for w in range(WORDS):
        word = jnp.int32(packed(0, w))
        for chip in range(1, CHIPS):
            word = jnp.where(own == chip, packed(chip, w), word)
        words.append(word)

    @pl.loop(0, STEPS)
    def _(n):
        at = n // PER_WORD
        word = words[0]
        for w in range(1, WORDS):
            word = jnp.where(at == w, words[w], word)
        event = jnp.right_shift(word, BITS * (n - at * PER_WORD)) % (1 << BITS)
        m = (event // 4) % CHIPS
        low = event % 4

        @pl.when(event < 32)
        def _():
            across(m, low).wait_recv()
            forward(m, low)

        @pl.when(jnp.logical_and(event >= 32, event < NOTHING))
        def _():
            @pl.when(low == 0)
            def _():
                arrived(m, (0, 1))

            @pl.when(jnp.logical_and(low == 0, m >= own))
            def _():
                arrived(m, (2, 3))

            @pl.when(m > own)
            def _():
                for i in range(2):
                    attend(L, 2 * low + i, m, [(E, 0), (L, 0)])

            @pl.when(m < own)
            def _():
                for i in range(2):
                    attend(E, 2 * low + i, m, [(E, 0)])
                    attend(L, 2 * low + i, m, [(E, 0)])

            @pl.when(m == own)
            def _():
                for i in range(2):
                    attend(E, 2 * low + i, m, [(E, 1)])
                    attend(L, 2 * low + i, m, [(L, 2), (E, 0)])

    back = jnp.transpose(perm[...].astype(F32), (1, 0))
    back_b = back.astype(BF16)
    logs = [[None] * QH, [None] * QH]
    for h in range(KVH):
        outs = []
        for part in (E, L):
            total = lst[part, h]
            outs.append((acc[part, h] / total).astype(BF16))
            log = mst[part, h] * LN2 + jnp.log(total)
            for g in range(GROUP):
                logs[part][h * GROUP + g] = log[:, g * HALF:(g + 1) * HALF]
        for g in range(GROUP):
            cols = slice(g * HALF, (g + 1) * HALF)
            both = jnp.concatenate([outs[0][:, cols], outs[1][:, cols]], axis=1)
            o_ref[h * GROUP + g] = dot(back_b, both, ((1,), (1,))).astype(BF16)
    lse = jnp.concatenate([jnp.concatenate(logs[0], axis=0), jnp.concatenate(logs[1], axis=0)], axis=1)
    lse_ref[...] = dot(back, lse, ((1,), (1,)), precision=lax.Precision.HIGHEST)

    @pl.loop(0, CHIPS * PARTS)
    def _(i):
        m = i // PARTS
        part = i % PARTS
        go_down, go_across, go_up = routes(m, part)

        @pl.when((part < 2) | (m >= own))
        def _():
            partner(m, part).wait_send()

            @pl.when(go_down)
            def _():
                down(m, part).wait_send()

            @pl.when(go_across)
            def _():
                across(m, part).wait_send()

            @pl.when(go_up)
            def _():
                up(m, part).wait_send()


def solution(mesh):
    half = np.arange(D // 2, dtype=np.float32) * np.float32(2.0) / np.float32(D)
    freq = np.power(np.float64(THETA), -half.astype(np.float64)).astype(np.float32)
    freq = np.concatenate([freq, freq])[None, :]

    def per_device(q_raw, k_raw, v_raw, positions, seq_ids, q_gain, k_gain):
        vmem = pl.BlockSpec(memory_space=pltpu.VMEM)
        sem = pltpu.SemaphoreType.DMA((CHIPS, PARTS))
        out, lse = pl.pallas_call(
            kernel,
            out_shape=(jax.ShapeDtypeStruct((QH, T, D), BF16), jax.ShapeDtypeStruct((T, QH), F32)),
            in_specs=[vmem] * 8,
            out_specs=(vmem, vmem),
            scratch_shapes=[
                pltpu.VMEM((CHIPS, PARTS, KVH, 2, HALF, D), BF16),
                pltpu.VMEM((2, KVH, D, GROUP * HALF), BF16),
                pltpu.VMEM((2, KVH, D, GROUP * HALF), F32),
                pltpu.VMEM((2, KVH, 1, GROUP * HALF), F32),
                pltpu.VMEM((2, KVH, 1, GROUP * HALF), F32),
                pltpu.VMEM((3, 2 * HALF, HALF), F32),
                pltpu.VMEM((2, T, D), F32),
                pltpu.VMEM((T, T), BF16),
                sem, sem, sem, sem, sem, sem,
            ],
            compiler_params=pltpu.CompilerParams(collective_id=0, has_side_effects=True, vmem_limit_bytes=48 * 1024 * 1024),
            name="gather_attend",
        )(q_raw, k_raw, v_raw, positions[None, :], seq_ids[None, :], q_gain[None, :], k_gain[None, :], jnp.asarray(freq))
        return jnp.transpose(out, (1, 0, 2)), lse

    return jax.shard_map(per_device, mesh=mesh, in_specs=(P("cp", "tp", None), P("cp", "tp", None), P("cp", "tp", None), P("cp"), P("cp"), P(), P()), out_specs=(P("cp", "tp", None), P("cp", "tp")), check_vma=False)
```

```python
import functools
import math

import jax
import jax.numpy as jnp
import numpy as np
from jax import lax
from jax.experimental import pallas as pl
from jax.experimental.pallas import tpu as pltpu
from jax.sharding import PartitionSpec as P

THETA = 1000000.0
EPS = 1e-6
NEG = -1e30
LAYERS = 4
CHIPS = 8
CP = 16
T = 256
HALF = 128
KVH = 4
GROUP = 4
QH = KVH * GROUP
D = 128
LOG2E = math.log2(math.e)
LN2 = math.log(2.0)
SCALE2 = D ** -0.5 * LOG2E
EVENTS = (
    (32, 33, 4, 8, 5, 9, 6, 10, 36, 40, 7, 11, 37, 41, 12, 16, 13, 17, 14, 18, 44, 48, 15, 19, 45, 49, 20, 24, 21, 25, 22, 26, 52, 56, 23, 27, 53, 57, 28, 30, 60, 29, 31, 61),
    (36, 37, 0, 12, 32, 1, 13, 33, 14, 8, 44, 15, 9, 45, 20, 10, 40, 21, 11, 41, 22, 16, 52, 23, 17, 53, 28, 18, 48, 29, 19, 49, 30, 24, 60, 31, 25, 61, 26, 56, 27, 57),
    (40, 41, 0, 12, 16, 32, 1, 13, 17, 33, 14, 18, 44, 48, 15, 19, 45, 49, 4, 24, 36, 20, 25, 5, 26, 37, 56, 21, 27, 57, 28, 22, 52, 29, 23, 53, 30, 60, 31, 61),
    (44, 45, 4, 8, 20, 36, 5, 9, 21, 40, 37, 41, 22, 0, 52, 23, 16, 32, 53, 28, 1, 33, 29, 17, 30, 18, 60, 48, 31, 19, 61, 49, 24, 25, 26, 56, 27, 57),
    (48, 49, 8, 20, 24, 40, 9, 21, 25, 41, 22, 26, 0, 52, 32, 23, 27, 1, 56, 53, 33, 12, 28, 57, 44, 13, 29, 45, 30, 60, 4, 36, 31, 61, 5, 37),
    (52, 53, 12, 16, 28, 44, 13, 17, 29, 48, 45, 49, 30, 4, 8, 60, 31, 24, 5, 36, 40, 37, 9, 61, 41, 25, 26, 56, 0, 32, 27, 57, 1, 33),
    (56, 57, 16, 28, 48, 17, 29, 49, 30, 8, 60, 40, 31, 9, 61, 41, 20, 0, 52, 32, 21, 1, 53, 12, 33, 44, 13, 45, 4, 36, 5, 37),
    (60, 61, 20, 24, 52, 21, 25, 56, 53, 57, 12, 16, 44, 48, 13, 17, 45, 4, 8, 49, 36, 40, 5, 9, 37, 41, 0, 32, 1, 33),
)
NOTHING = 64
STEPS = max(len(e) for e in EVENTS)
BITS = 7
PER_WORD = 4
WORDS = -(-STEPS // PER_WORD)
PARTS = 4


def packed(chip, word):
    events = EVENTS[chip] + (NOTHING,) * (WORDS * PER_WORD)
    return sum(events[word * PER_WORD + i] << (BITS * i) for i in range(PER_WORD))


E, L = 0, 1
F32 = jnp.float32
BF16 = jnp.bfloat16
MESH = pl.DeviceIdType.MESH


def dot(a, b, dims, precision=None):
    return lax.dot_general(a, b, (dims, ((), ())), preferred_element_type=F32, precision=precision)


def column(row, ident):
    return jnp.sum(jnp.where(ident, row, 0.0), axis=1, keepdims=True)


def norm_rope(x, gain, cos, sin):
    inv = lax.rsqrt(jnp.mean(x * x, axis=-1, keepdims=True) + EPS)
    normed = (x * inv * gain).astype(BF16).astype(F32)
    return (normed * cos + pltpu.roll(normed, D // 2, 1) * sin).astype(BF16)


def kernel(q_hbm, k_hbm, v_hbm, pos_hbm, seq_hbm, qg_hbm, kg_hbm, freq_hbm, o_ref, lse_ref,
           kvbuf, qbuf, acc, mst, lst, bias, sbuf, pbuf, rope, perm,
           q_in, k_in, v_in, pos_ref, seq_ref, qg_ref, kg_ref, freq_ref,
           s_dn, s_up, s_y, s_d, r_link, r_d, s_in):
    me = lax.axis_index("cp")
    z = me // 4
    y = (me // 2) % 2
    c = me % 2
    own = me // 2

    def dev(zz, yy, cc):
        return {"cp": zz * 4 + yy * 2 + cc}

    barrier = pltpu.get_barrier_semaphore()
    pl.semaphore_signal(barrier, inc=1, device_id=dev(z, y, 1 - c), device_id_type=MESH)
    pl.semaphore_signal(barrier, inc=1, device_id=dev(z, 1 - y, c), device_id_type=MESH)

    @pl.when(z > 0)
    def _():
        pl.semaphore_signal(barrier, inc=1, device_id=dev(z - 1, y, c), device_id_type=MESH)

    @pl.when(z < LAYERS - 1)
    def _():
        pl.semaphore_signal(barrier, inc=1, device_id=dev(z + 1, y, c), device_id_type=MESH)

    pairs = ((pos_hbm, pos_ref), (seq_hbm, seq_ref), (freq_hbm, freq_ref), (kg_hbm, kg_ref), (k_hbm, k_in), (v_hbm, v_in),
             (qg_hbm, qg_ref), (q_hbm, q_in))
    loads = [pltpu.make_async_copy(src, dst, s_in.at[i]) for i, (src, dst) in enumerate(pairs)]
    for load in loads:
        load.start()
    loads[0].wait()
    loads[1].wait()

    row_i = lax.broadcasted_iota(jnp.int32, (T, T), 0)
    col_i = lax.broadcasted_iota(jnp.int32, (T, T), 1)
    ident = row_i == col_i
    pos_row = pos_ref[...].astype(F32)
    seq_row = seq_ref[...].astype(F32)
    pos_col = column(pos_row, ident)
    seq_col = column(seq_row, ident)
    same = (seq_col == seq_row).astype(F32)
    early_row = (pos_row < 8.0 * jnp.sum(same, axis=0, keepdims=True)).astype(F32)
    early_col = (pos_col < 8.0 * jnp.sum(same, axis=1, keepdims=True)).astype(F32)
    alike = (early_col == early_row).astype(F32)
    dest_row = jnp.sum(jnp.where(row_i < col_i, alike, 0.0), axis=0, keepdims=True) + HALF * (1.0 - early_row)
    one_hot = (row_i.astype(F32) == dest_row).astype(BF16)
    perm[...] = one_hot

    left = lax.broadcasted_iota(jnp.int32, (HALF, D), 1) < D // 2
    loads[2].wait()
    angle = jnp.where(left, pos_col[:HALF], pos_col[HALF:]) * freq_ref[...]
    cos = jnp.cos(angle)
    sin = jnp.sin(angle)
    cos_r = pltpu.roll(cos, D // 2, 1)
    sin_r = pltpu.roll(sin, D // 2, 1)
    cos = jnp.concatenate([jnp.where(left, cos, cos_r), jnp.where(left, cos_r, cos)], axis=0)
    sin = jnp.concatenate([jnp.where(left, -sin, sin_r), jnp.where(left, -sin_r, sin)], axis=0)
    rope[0] = cos
    rope[1] = sin

    loads[3].wait()
    loads[4].wait()
    loads[5].wait()
    k_all = jnp.transpose(k_in[...].astype(F32), (1, 0, 2))
    v_all = jnp.transpose(v_in[...].astype(F32), (1, 0, 2)).astype(BF16)
    gain = kg_ref[...].astype(F32)
    for h in range(KVH):
        kr = dot(one_hot, norm_rope(k_all[h], gain, cos, sin), ((1,), (0,))).astype(BF16)
        vr = dot(v_all[h], one_hot, ((0,), (1,))).astype(BF16)
        for part in (E, L):
            kvbuf[own, 2 * part + h // 2, 0, h % 2, c] = kr[part * HALF:(part + 1) * HALF]
            kvbuf[own, 2 * part + h // 2, 1, h % 2, c] = vr[:, part * HALF:(part + 1) * HALF]

    pl.semaphore_wait(barrier, 2 + jnp.minimum(z, 1) + jnp.minimum(LAYERS - 1 - z, 1))

    def copy(m, part, send, recv, target):
        ref = kvbuf.at[m, part, :, :, c]
        return pltpu.make_async_remote_copy(
            src_ref=ref, dst_ref=ref, send_sem=send.at[m, part], recv_sem=recv.at[m, part],
            device_id=target, device_id_type=MESH)

    def down(m, part):
        return copy(m, part, s_dn, r_link, dev(z - 1, y, c))

    def up(m, part):
        return copy(m, part, s_up, r_link, dev(z + 1, y, c))

    def across(m, part):
        return copy(m, part, s_y, r_link, dev(z, 1 - y, c))

    def partner(m, part):
        return copy(m, part, s_d, r_d, dev(z, y, 1 - c))

    def routes(m, part):
        mz = m // 2
        straight = m % 2 == y
        early = part < 2
        both = jnp.logical_and(early, m == CHIPS - 1)
        go_down = (z > 0) & (mz >= z) & (straight | (both & (y == 0)))
        go_across = straight & jnp.where(early, ~(both & (z < LAYERS - 1)), m > z * 2 + 1 - y)
        go_up = early & (z < LAYERS - 1) & (mz <= z) & straight
        return go_down, go_across, go_up

    def forward(m, part):
        go_down, go_across, go_up = routes(m, part)

        @pl.when(go_down)
        def _():
            down(m, part).start()

        @pl.when(go_across)
        def _():
            across(m, part).start()

        @pl.when(go_up)
        def _():
            up(m, part).start()

        partner(m, part).start()

    @pl.loop(0, PARTS)
    def _(part):
        forward(own, part)

    loads[6].wait()
    loads[7].wait()
    q_all = jnp.transpose(q_in[...].astype(F32), (1, 0, 2))
    q_gain = qg_ref[...].astype(F32)
    for h in range(QH):
        qr = dot(norm_rope(q_all[h], q_gain, rope[0], rope[1]), perm[...], ((0,), (1,))).astype(BF16)
        for part in (E, L):
            qbuf[part, h // GROUP, :, (h % GROUP) * HALF:(h % GROUP + 1) * HALF] = qr[:, part * HALF:(part + 1) * HALF]

    seg = dot(perm[0:HALF], same.astype(BF16), ((1,), (0,))).astype(BF16)
    seg = dot(seg, perm[0:HALF], ((1,), (1,))) > 0.5
    r_i = lax.broadcasted_iota(jnp.int32, (HALF, HALF), 0)
    c_i = lax.broadcasted_iota(jnp.int32, (HALF, HALF), 1)
    full = jnp.where(seg, 0.0, NEG)
    diag = jnp.where(jnp.logical_and(seg, r_i <= c_i), 0.0, NEG)
    none = jnp.full((HALF, HALF), NEG, F32)
    first = c == 0
    bias[0, 0:HALF] = full
    bias[0, HALF:] = full
    bias[1, 0:HALF] = jnp.where(first, diag, full)
    bias[1, HALF:] = jnp.where(first, none, diag)
    bias[2, 0:HALF] = jnp.where(first, diag, none)
    bias[2, HALF:] = jnp.where(first, full, diag)

    mst[...] = jnp.full(mst.shape, NEG, F32)
    lst[...] = jnp.zeros(lst.shape, F32)
    acc[...] = jnp.zeros(acc.shape, F32)

    def attend(m, pair, units):
        def scores(i):
            qp, hh, part, _ = units[i]
            keys = kvbuf[m, 2 * part + pair, 0, hh].reshape(2 * HALF, D)
            sbuf[i % 2] = dot(keys, qbuf[qp, 2 * pair + hh], ((1,), (0,)))

        def weigh(i):
            qp, hh, _, b = units[i]
            h = 2 * pair + hh
            s = sbuf[i % 2] * SCALE2 + jnp.concatenate([bias[b]] * GROUP, axis=1)
            m_old = mst[qp, h]
            m_new = jnp.maximum(m_old, jnp.max(s, axis=0, keepdims=True))
            alpha = jnp.exp2(m_old - m_new)
            p = jnp.exp2(s - m_new)
            lst[qp, h] = lst[qp, h] * alpha + jnp.sum(p, axis=0, keepdims=True)
            mst[qp, h] = m_new
            pbuf[i % 2] = p.astype(BF16)
            return alpha

        def values(i, alpha):
            qp, hh, part, _ = units[i]
            h = 2 * pair + hh
            vals = kvbuf[m, 2 * part + pair, 1, hh]
            vals = jnp.concatenate([vals[0], vals[1]], axis=1)
            acc[qp, h] = acc[qp, h] * alpha + dot(vals, pbuf[i % 2], ((1,), (0,)))

        scores(0)
        alpha = None
        for i in range(len(units)):
            if i + 1 < len(units):
                scores(i + 1)
            previous, alpha = alpha, weigh(i)
            if i > 0:
                values(i - 1, previous)
        values(len(units) - 1, alpha)

    words = []
    for w in range(WORDS):
        word = jnp.int32(packed(0, w))
        for chip in range(1, CHIPS):
            word = jnp.where(own == chip, packed(chip, w), word)
        words.append(word)

    @pl.loop(0, STEPS)
    def _(n):
        at = n // PER_WORD
        word = words[0]
        for w in range(1, WORDS):
            word = jnp.where(at == w, words[w], word)
        event = jnp.right_shift(word, BITS * (n - at * PER_WORD)) % (1 << BITS)
        m = (event // 4) % CHIPS
        low = event % 4

        @pl.when(event < 32)
        def _():
            across(m, low).wait_recv()
            forward(m, low)

        @pl.when(jnp.logical_and(event >= 32, event < NOTHING))
        def _():
            partner(m, low).wait_recv()

            @pl.when(m >= own)
            def _():
                partner(m, 2 + low).wait_recv()

            @pl.when(m > own)
            def _():
                attend(m, low, [(L, 0, E, 0), (L, 1, E, 0), (L, 0, L, 0), (L, 1, L, 0)])

            @pl.when(m < own)
            def _():
                attend(m, low, [(E, 0, E, 0), (L, 0, E, 0), (E, 1, E, 0), (L, 1, E, 0)])

            @pl.when(m == own)
            def _():
                attend(m, low, [(E, 0, E, 1), (L, 0, L, 2), (E, 1, E, 1), (L, 1, L, 2), (L, 0, E, 0), (L, 1, E, 0)])

    back_b = jnp.transpose(perm[...].astype(F32), (1, 0)).astype(BF16)
    logs = [[None] * QH, [None] * QH]
    for h in range(KVH):
        outs = []
        for part in (E, L):
            total = lst[part, h]
            outs.append((acc[part, h] / total).astype(BF16))
            log = mst[part, h] * LN2 + jnp.log(total)
            for g in range(GROUP):
                logs[part][h * GROUP + g] = log[:, g * HALF:(g + 1) * HALF]
        for g in range(0, GROUP, 2):
            stack = []
            for i in (g, g + 1):
                cols = slice(i * HALF, (i + 1) * HALF)
                stack.append(jnp.concatenate([outs[0][:, cols], outs[1][:, cols]], axis=1))
            two = dot(back_b, jnp.concatenate(stack, axis=0), ((1,), (1,))).astype(BF16)
            o_ref[h * GROUP + g] = two[:, 0:D]
            o_ref[h * GROUP + g + 1] = two[:, D:]
    lse = jnp.concatenate([jnp.concatenate(logs[0], axis=0), jnp.concatenate(logs[1], axis=0)], axis=1)
    lse_ref[...] = dot(lse, perm[...].astype(F32), ((1,), (0,)), precision=lax.Precision.HIGHEST)

    @pl.loop(0, CHIPS * PARTS)
    def _(i):
        m = i // PARTS
        part = i % PARTS
        go_down, go_across, go_up = routes(m, part)

        @pl.when((part < 2) | (m >= own))
        def _():
            partner(m, part).wait_send()

            @pl.when(go_down)
            def _():
                down(m, part).wait_send()

            @pl.when(go_across)
            def _():
                across(m, part).wait_send()

            @pl.when(go_up)
            def _():
                up(m, part).wait_send()


def solution(mesh):
    half = np.arange(D // 2, dtype=np.float32) * np.float32(2.0) / np.float32(D)
    freq = np.power(np.float64(THETA), -half.astype(np.float64)).astype(np.float32)
    freq = np.concatenate([freq, freq])[None, :]

    def per_device(q_raw, k_raw, v_raw, positions, seq_ids, q_gain, k_gain):
        vmem = pl.BlockSpec(memory_space=pltpu.VMEM)
        hbm = pl.BlockSpec(memory_space=pltpu.HBM)
        sem = pltpu.SemaphoreType.DMA((CHIPS, PARTS))
        inputs = (q_raw, k_raw, v_raw, positions[None, :], seq_ids[None, :], q_gain[None, :], k_gain[None, :], jnp.asarray(freq))
        out, lse = pl.pallas_call(
            kernel,
            out_shape=(jax.ShapeDtypeStruct((QH, T, D), BF16), jax.ShapeDtypeStruct((QH, T), F32)),
            in_specs=[hbm] * 8,
            out_specs=(vmem, vmem),
            scratch_shapes=[
                pltpu.VMEM((CHIPS, PARTS, 2, 2, 2, HALF, D), BF16),
                pltpu.VMEM((2, KVH, D, GROUP * HALF), BF16),
                pltpu.VMEM((2, KVH, D, GROUP * HALF), F32),
                pltpu.VMEM((2, KVH, 1, GROUP * HALF), F32),
                pltpu.VMEM((2, KVH, 1, GROUP * HALF), F32),
                pltpu.VMEM((3, 2 * HALF, HALF), F32),
                pltpu.VMEM((2, 2 * HALF, GROUP * HALF), F32),
                pltpu.VMEM((2, 2 * HALF, GROUP * HALF), BF16),
                pltpu.VMEM((2, T, D), F32),
                pltpu.VMEM((T, T), BF16),
                pltpu.VMEM((T, QH, D), BF16),
                pltpu.VMEM((T, KVH, D), BF16),
                pltpu.VMEM((T, KVH, D), BF16),
                pltpu.VMEM((1, T), jnp.int32),
                pltpu.VMEM((1, T), jnp.int32),
                pltpu.VMEM((1, D), BF16),
                pltpu.VMEM((1, D), BF16),
                pltpu.VMEM((1, D), F32),
                sem, sem, sem, sem, sem, sem,
                pltpu.SemaphoreType.DMA((8,)),
            ],
            compiler_params=pltpu.CompilerParams(collective_id=0, has_side_effects=True, vmem_limit_bytes=48 * 1024 * 1024),
            name="gather_attend",
        )(*[pltpu.with_memory_space_constraint(x, pltpu.HBM) for x in inputs])
        return jnp.transpose(out, (1, 0, 2)), lse.T

    return jax.shard_map(per_device, mesh=mesh, in_specs=(P("cp", "tp", None), P("cp", "tp", None), P("cp", "tp", None), P("cp"), P("cp"), P(), P()), out_specs=(P("cp", "tp", None), P("cp", "tp")), check_vma=False)
```

```python
import functools
import math

import jax
import jax.numpy as jnp
import numpy as np
from jax import lax
from jax.experimental import pallas as pl
from jax.experimental.pallas import tpu as pltpu
from jax.sharding import PartitionSpec as P

THETA = 1000000.0
EPS = 1e-6
NEG = -1e30
LAYERS = 4
CHIPS = 8
CP = 16
T = 256
HALF = 128
KVH = 4
GROUP = 4
QH = KVH * GROUP
D = 128
LOG2E = math.log2(math.e)
LN2 = math.log(2.0)
SCALE2 = D ** -0.5 * LOG2E
EVENTS = (
    (64, 65, 8, 18, 9, 11, 16, 80, 10, 34, 72, 26, 32, 96, 24, 48, 88, 42, 50, 112, 40, 104, 58, 56, 120, 132, 133),
    (72, 73, 0, 26, 64, 1, 24, 65, 88, 18, 42, 16, 80, 40, 34, 104, 56, 32, 96, 58, 48, 120, 50, 112, 133, 132),
    (81, 80, 0, 26, 34, 1, 25, 33, 64, 3, 27, 35, 65, 89, 130, 144, 24, 32, 9, 152, 97, 41, 11, 160, 73, 136, 48, 88, 8, 96, 50, 72, 42, 49, 112, 51, 113, 40, 176, 43, 56, 104, 59, 57, 105, 168, 121, 184, 129, 58, 133, 120, 132),
    (89, 17, 41, 88, 19, 8, 81, 9, 42, 72, 16, 11, 73, 80, 40, 34, 43, 138, 1, 144, 152, 0, 33, 65, 128, 56, 35, 105, 168, 59, 97, 160, 64, 32, 58, 104, 57, 96, 48, 49, 51, 121, 184, 113, 176, 50, 129, 120, 112, 133, 132),
    (96, 17, 41, 48, 97, 81, 16, 42, 80, 50, 40, 49, 112, 0, 43, 51, 1, 104, 25, 64, 9, 24, 56, 57, 59, 65, 73, 88, 89, 58, 105, 113, 120, 121, 8, 133, 72, 132),
    (104, 25, 33, 56, 105, 89, 24, 32, 59, 97, 17, 88, 81, 58, 48, 96, 8, 57, 120, 9, 16, 72, 73, 80, 50, 121, 49, 0, 112, 51, 64, 1, 113, 132, 65, 133),
    (112, 33, 113, 56, 97, 32, 59, 17, 96, 41, 81, 58, 105, 120, 57, 16, 121, 80, 40, 104, 0, 1, 24, 65, 25, 64, 9, 88, 8, 73, 89, 72, 133, 132),
    (120, 41, 121, 48, 105, 40, 49, 112, 25, 33, 104, 89, 97, 113, 32, 24, 17, 96, 81, 88, 8, 16, 72, 9, 80, 1, 73, 65, 133, 0, 64, 132),
)
ROUTES = (
    (2102, 2080, 130, 0, 130, 0, 130, 0),
    (4, 3254, 0, 130, 0, 130, 0, 128),
    (52, 32, 1143, 32, 1235, 0, 195, 1),
    (4, 38, 32, 1271, 0, 1235, 0, 1217),
    (52, 32, 38, 32, 639, 32, 1755, 9),
    (4, 38, 32, 38, 0, 1791, 520, 1737),
    (16, 0, 2, 0, 18, 0, 603, 9),
    (0, 2, 0, 2, 0, 2, 0, 1755),
)
HOLDS = (
    (15, 5, 5, 5, 5, 5, 5, 5),
    (3, 15, 5, 5, 5, 5, 5, 5),
    (11, 11, 15, 15, 15, 15, 15, 15),
    (3, 11, 11, 15, 15, 15, 15, 15),
    (3, 3, 3, 3, 15, 15, 15, 15),
    (3, 3, 3, 3, 3, 15, 15, 15),
    (3, 3, 3, 3, 3, 3, 15, 15),
    (3, 3, 3, 3, 3, 3, 3, 15),
)
FIRST = (
    (2, 0, 1, 3),
    (0, 1, 3, 2),
    (1, 2, 3, 0),
    (2, 1, 3, 0),
    (2, 1, 3, 0),
    (1, 2, 0, 3),
    (0, 2, 1, 3),
    (0, 3, 2, 1),
)
GUEST = 2
NOTHING = 255
STEPS = max(len(e) for e in EVENTS)
BITS = 8
PER_WORD = 4
WORDS = -(-STEPS // PER_WORD)
PARTS = 4
GROUPS = ((0, 1, 2), (3,))


def pack(fields, bits):
    word = sum(f << (bits * i) for i, f in enumerate(fields))
    return word - (1 << 32) if word >= 1 << 31 else word


def event_word(chip, word):
    events = EVENTS[chip] + (NOTHING,) * (WORDS * PER_WORD)
    return pack(events[word * PER_WORD:(word + 1) * PER_WORD], BITS)


def route_word(chip, pair):
    return pack([ROUTES[chip][m] + (HOLDS[chip][m] << (3 * PARTS)) for m in (2 * pair, 2 * pair + 1)], 16)


def select(index, values):
    values = [jnp.int32(v) if isinstance(v, int) else v for v in values]
    while len(values) > 1:
        odd = index % 2 == 1
        values = [jnp.where(odd, values[i + 1], values[i]) if i + 1 < len(values) else values[i] for i in range(0, len(values), 2)]
        index = index // 2
    return values[0]


E, L = 0, 1
F32 = jnp.float32
BF16 = jnp.bfloat16
MESH = pl.DeviceIdType.MESH


def dot(a, b, dims, precision=None):
    return lax.dot_general(a, b, (dims, ((), ())), preferred_element_type=F32, precision=precision)


def column(row, ident):
    return jnp.sum(jnp.where(ident, row, 0.0), axis=1, keepdims=True)


def norm_rope(x, gain, cos, sin):
    inv = lax.rsqrt(jnp.mean(x * x, axis=-1, keepdims=True) + EPS)
    normed = (x * inv * gain).astype(BF16).astype(F32)
    return (normed * cos + pltpu.roll(normed, D // 2, 1) * sin).astype(BF16)


def kernel(q_hbm, k_hbm, v_hbm, pos_hbm, seq_hbm, qg_hbm, kg_hbm, freq_hbm, o_ref, lse_ref,
           kvbuf, qbuf, acc, mst, lst, bias, rope, perm,
           q_in, k_in, v_in, pos_ref, seq_ref, qg_ref, kg_ref, freq_ref,
           s_dn, s_up, s_y, s_d, r_link, r_d, s_in, s_x, r_x,
           perm_t, logs, x_out, x_log):
    me = lax.axis_index("cp")
    z = me // 4
    y = (me // 2) % 2
    c = me % 2
    own = me // 2

    def dev(zz, yy, cc):
        return {"cp": zz * 4 + yy * 2 + cc}

    barrier = pltpu.get_barrier_semaphore()
    pl.semaphore_signal(barrier, inc=1, device_id=dev(z, y, 1 - c), device_id_type=MESH)
    pl.semaphore_signal(barrier, inc=1, device_id=dev(z, 1 - y, c), device_id_type=MESH)

    @pl.when(z > 0)
    def _():
        pl.semaphore_signal(barrier, inc=1, device_id=dev(z - 1, y, c), device_id_type=MESH)

    @pl.when(z < LAYERS - 1)
    def _():
        pl.semaphore_signal(barrier, inc=1, device_id=dev(z + 1, y, c), device_id_type=MESH)

    pairs = ((pos_hbm, pos_ref), (seq_hbm, seq_ref), (freq_hbm, freq_ref), (kg_hbm, kg_ref), (k_hbm, k_in), (v_hbm, v_in),
             (qg_hbm, qg_ref), (q_hbm, q_in))
    loads = [pltpu.make_async_copy(src, dst, s_in.at[i]) for i, (src, dst) in enumerate(pairs)]
    for load in loads:
        load.start()
    loads[0].wait()
    loads[1].wait()

    row_i = lax.broadcasted_iota(jnp.int32, (T, T), 0)
    col_i = lax.broadcasted_iota(jnp.int32, (T, T), 1)
    ident = row_i == col_i
    pos_row = pos_ref[...].astype(F32)
    seq_row = seq_ref[...].astype(F32)
    pos_col = column(pos_row, ident)
    seq_col = column(seq_row, ident)
    same = (seq_col == seq_row).astype(F32)
    early_row = (pos_row < 8.0 * jnp.sum(same, axis=0, keepdims=True)).astype(F32)
    early_col = (pos_col < 8.0 * jnp.sum(same, axis=1, keepdims=True)).astype(F32)
    alike = (early_col == early_row).astype(F32)
    dest_row = jnp.sum(jnp.where(row_i < col_i, alike, 0.0), axis=0, keepdims=True) + HALF * (1.0 - early_row)
    one_hot = (row_i.astype(F32) == dest_row).astype(BF16)
    perm[...] = one_hot

    left = lax.broadcasted_iota(jnp.int32, (HALF, D), 1) < D // 2
    loads[2].wait()
    angle = jnp.where(left, pos_col[:HALF], pos_col[HALF:]) * freq_ref[...]
    cos = jnp.cos(angle)
    sin = jnp.sin(angle)
    cos_r = pltpu.roll(cos, D // 2, 1)
    sin_r = pltpu.roll(sin, D // 2, 1)
    cos = jnp.concatenate([jnp.where(left, cos, cos_r), jnp.where(left, cos_r, cos)], axis=0)
    sin = jnp.concatenate([jnp.where(left, -sin, sin_r), jnp.where(left, -sin_r, sin)], axis=0)
    rope[0] = cos
    rope[1] = sin

    loads[3].wait()
    loads[4].wait()
    loads[5].wait()
    k_all = jnp.transpose(k_in[...].astype(F32), (1, 0, 2))
    v_all = jnp.transpose(v_in[...].astype(F32), (1, 0, 2)).astype(BF16)
    gain = kg_ref[...].astype(F32)
    for h in range(KVH):
        kr = dot(one_hot, norm_rope(k_all[h], gain, cos, sin), ((1,), (0,))).astype(BF16)
        vr = dot(v_all[h], one_hot, ((0,), (1,))).astype(BF16)
        for part in (E, L):
            kvbuf[own, part, h, 0, c] = kr[part * HALF:(part + 1) * HALF]
            kvbuf[own, part, h, 1, c] = vr[:, part * HALF:(part + 1) * HALF]

    pl.semaphore_wait(barrier, 2 + jnp.minimum(z, 1) + jnp.minimum(LAYERS - 1 - z, 1))

    class Copy:
        def __init__(self, m, part, send, recv, target):
            self.args = (m, part, send, recv, target)

        def act(self, name):
            m, part, send, recv, target = self.args

            def run(g):
                ref = kvbuf.at[m, part // 2, pl.ds(GROUPS[g][0], len(GROUPS[g])), :, c]
                getattr(pltpu.make_async_remote_copy(
                    src_ref=ref, dst_ref=ref, send_sem=send.at[m, part], recv_sem=recv.at[m, part],
                    device_id=target, device_id_type=MESH), name)()

            if isinstance(part, int):
                run(part % 2)
            else:
                pl.when(part % 2 == 0)(lambda: run(0))
                pl.when(part % 2 == 1)(lambda: run(1))

        def start(self):
            self.act("start")

        def wait_recv(self):
            self.act("wait_recv")

        def wait_send(self):
            self.act("wait_send")

    def down(m, part):
        return Copy(m, part, s_dn, r_link, dev(z - 1, y, c))

    def up(m, part):
        return Copy(m, part, s_up, r_link, dev(z + 1, y, c))

    def across(m, part):
        return Copy(m, part, s_y, r_link, dev(z, 1 - y, c))

    def partner(m, part):
        return Copy(m, part, s_d, r_d, dev(z, y, 1 - c))

    route_words = [select(own, [route_word(chip, pair) for chip in range(CHIPS)]) for pair in range(CHIPS // 2)]
    event_words = [select(own, [event_word(chip, w) for chip in range(CHIPS)]) for w in range(WORDS)]
    first_word = select(own, [sum(p << (3 * i) for i, p in enumerate(row)) for row in FIRST])

    def routes(m, part):
        entry = jnp.right_shift(select(m // 2, route_words), 16 * (m % 2))
        way = jnp.right_shift(entry, 3 * part) % 8
        need = jnp.right_shift(entry, 3 * PARTS + part) % 2
        return way % 2 == 1, (way // 2) % 2 == 1, way // 4 == 1, need == 1

    def forward(m, part):
        go_down, go_across, go_up, go_partner = routes(m, part)

        @pl.when(go_down)
        def _():
            down(m, part).start()

        @pl.when(go_across)
        def _():
            across(m, part).start()

        @pl.when(go_up)
        def _():
            up(m, part).start()

        @pl.when(go_partner)
        def _():
            partner(m, part).start()

    @pl.loop(0, PARTS)
    def _(i):
        forward(own, jnp.right_shift(first_word, 3 * i) % 8)

    loads[6].wait()
    loads[7].wait()
    q_all = jnp.transpose(q_in[...].astype(F32), (1, 0, 2))
    q_gain = qg_ref[...].astype(F32)
    for h in range(QH):
        qr = dot(norm_rope(q_all[h], q_gain, rope[0], rope[1]), perm[...], ((0,), (1,))).astype(BF16)
        for part in (E, L):
            qbuf[part, h // GROUP, :, (h % GROUP) * HALF:(h % GROUP + 1) * HALF] = qr[:, part * HALF:(part + 1) * HALF]

    def ship(i, src, dst, zz):
        return pltpu.make_async_remote_copy(
            src_ref=src, dst_ref=dst, send_sem=s_x.at[i], recv_sem=r_x.at[i], device_id=dev(zz, y, c), device_id_type=MESH)

    def ship_queries():
        return ship(0, qbuf.at[L, KVH - 1], qbuf.at[GUEST, KVH - 1], 1 - z)

    def ship_results():
        return ship(1, x_out, x_out, 1 - z), ship(2, x_log, x_log, 1 - z)

    seg = dot(perm[0:HALF], same.astype(BF16), ((1,), (0,))).astype(BF16)
    seg = dot(seg, perm[0:HALF], ((1,), (1,))) > 0.5
    r_i = lax.broadcasted_iota(jnp.int32, (HALF, HALF), 0)
    c_i = lax.broadcasted_iota(jnp.int32, (HALF, HALF), 1)
    full = jnp.where(seg, 0.0, NEG)
    diag = jnp.where(jnp.logical_and(seg, r_i <= c_i), 0.0, NEG)
    none = jnp.full((HALF, HALF), NEG, F32)
    first = c == 0
    bias[0, 0:HALF] = full
    bias[0, HALF:] = full
    bias[1, 0:HALF] = jnp.where(first, diag, full)
    bias[1, HALF:] = jnp.where(first, none, diag)
    bias[2, 0:HALF] = jnp.where(first, diag, none)
    bias[2, HALF:] = jnp.where(first, full, diag)

    @pl.when(z == 0)
    def _():
        ship_queries().start()

    mst[...] = jnp.full(mst.shape, NEG, F32)
    lst[...] = jnp.zeros(lst.shape, F32)
    acc[...] = jnp.zeros(acc.shape, F32)

    def attend(m, heads, groups):
        work = [(h, qp, keys) for h in heads for qp, keys in groups]
        scores = []
        for h, qp, keys in work:
            q = qbuf[qp, h]
            scores.append([dot(kvbuf[m, piece, h, 0].reshape(2 * HALF, D), q, ((1,), (0,))) for piece, _ in keys])
        for (h, qp, keys), group in zip(work, scores):
            group = [s * SCALE2 + jnp.concatenate([bias[b]] * GROUP, axis=1) for s, (_, b) in zip(group, keys)]
            m_old = mst[qp, h]
            m_new = m_old
            for s in group:
                m_new = jnp.maximum(m_new, jnp.max(s, axis=0, keepdims=True))
            alpha = jnp.exp2(m_old - m_new)
            total = lst[qp, h] * alpha
            out = acc[qp, h] * alpha
            for s, (piece, _) in zip(group, keys):
                p = jnp.exp2(s - m_new)
                total = total + jnp.sum(p, axis=0, keepdims=True)
                vals = kvbuf[m, piece, h, 1]
                out = out + dot(jnp.concatenate([vals[0], vals[1]], axis=1), p.astype(BF16), ((1,), (0,)))
            mst[qp, h] = m_new
            lst[qp, h] = total
            acc[qp, h] = out

    back = jnp.transpose(perm[...].astype(F32), (1, 0)).astype(BF16)
    perm_t[...] = back

    def finish(h):
        outs = []
        for part in (E, L):
            total = lst[part, h]
            out = (acc[part, h] / total).astype(BF16)
            log = mst[part, h] * LN2 + jnp.log(total)
            outs.append(out)
            logs[h, :, part * GROUP * HALF:(part + 1) * GROUP * HALF] = log
        for g in range(0, GROUP, 2):
            stack = []
            for i in (g, g + 1):
                cols = slice(i * HALF, (i + 1) * HALF)
                stack.append(jnp.concatenate([outs[0][:, cols], outs[1][:, cols]], axis=1))
            two = dot(perm_t[...], jnp.concatenate(stack, axis=0), ((1,), (1,))).astype(BF16)
            o_ref[h * GROUP + g] = two[:, 0:D]
            o_ref[h * GROUP + g + 1] = two[:, D:]

    def step(event):
        kind = event // 64
        m = (event // 8) % CHIPS
        low = event % 8

        @pl.when(kind == 0)
        def _():
            across(m, low).wait_recv()
            forward(m, low)

        for g, heads in enumerate(GROUPS):
            @pl.when(jnp.logical_and(kind == 1, low == g))
            def _():
                partner(m, g).wait_recv()

                @pl.when(m >= own)
                def _():
                    partner(m, 2 + g).wait_recv()

                away = z == 0 if g == 1 else z < 0
                here = jnp.logical_not(away)

                @pl.when(jnp.logical_and(here, m > own))
                def _():
                    attend(m, heads, [(L, [(E, 0), (L, 0)])])

                @pl.when(jnp.logical_and(here, m < own))
                def _():
                    attend(m, heads, [(E, [(E, 0)]), (L, [(E, 0)])])

                @pl.when(jnp.logical_and(here, m == own))
                def _():
                    attend(m, heads, [(E, [(E, 1)]), (L, [(L, 2), (E, 0)])])

                if g == 1:
                    @pl.when(away)
                    def _():
                        attend(m, heads, [(E, [(E, jnp.where(m == own, 1, 0))])])

        @pl.when(jnp.logical_and(kind == 2, jnp.logical_or(low == 0, low == 2)))
        def _():
            @pl.when(low == 2)
            def _():
                ship_queries().wait_recv()

            @pl.when(jnp.logical_and(m >= y, m < own))
            def _():
                partner(m, PARTS - 1).wait_recv()

            @pl.when(m >= y)
            def _():
                attend(m, GROUPS[1], [(GUEST, [(E, 0), (L, jnp.where(m == y, 2, 0))])])

            @pl.when(m < y)
            def _():
                attend(m, GROUPS[1], [(GUEST, [(E, 0)])])

        @pl.when(jnp.logical_and(kind == 2, low == 1))
        def _():
            total = lst[GUEST, KVH - 1]
            x_out[...] = (acc[GUEST, KVH - 1] / total).astype(BF16)
            x_log[...] = mst[GUEST, KVH - 1] * LN2 + jnp.log(total)
            for x in ship_results():
                x.start()

        @pl.when(jnp.logical_and(kind == 2, low == 4))
        def _():
            for h in GROUPS[0]:
                finish(h)

        @pl.when(jnp.logical_and(kind == 2, low == 5))
        def _():
            @pl.when(z == 0)
            def _():
                for x in ship_results():
                    x.wait_recv()
                acc[L, KVH - 1] = x_out[...].astype(F32)
                lst[L, KVH - 1] = jnp.ones((1, GROUP * HALF), F32)
                mst[L, KVH - 1] = x_log[...] * LOG2E

            finish(KVH - 1)

    @pl.loop(0, WORDS)
    def _(n):
        word = select(n, event_words)

        @pl.loop(0, PER_WORD)
        def _(i):
            step(jnp.right_shift(word, BITS * i) % (1 << BITS))

    lse = []
    for part in (E, L):
        rows = []
        for h in range(KVH):
            for g in range(GROUP):
                at = (part * GROUP + g) * HALF
                rows.append(logs[h, :, at:at + HALF])
        lse.append(jnp.concatenate(rows, axis=0))
    lse = jnp.concatenate(lse, axis=1)
    lse_ref[...] = dot(lse, perm[...].astype(F32), ((1,), (0,)), precision=lax.Precision.HIGHEST)

    @pl.loop(0, CHIPS * PARTS)
    def _(i):
        m = i // PARTS
        part = i % PARTS
        go_down, go_across, go_up, go_partner = routes(m, part)

        @pl.when(go_partner)
        def _():
            partner(m, part).wait_send()

        @pl.when(go_down)
        def _():
            down(m, part).wait_send()

        @pl.when(go_across)
        def _():
            across(m, part).wait_send()

        @pl.when(go_up)
        def _():
            up(m, part).wait_send()

    @pl.when(z == 0)
    def _():
        ship_queries().wait_send()

    @pl.when(z == 1)
    def _():
        for x in ship_results():
            x.wait_send()


def solution(mesh):
    half = np.arange(D // 2, dtype=np.float32) * np.float32(2.0) / np.float32(D)
    freq = np.power(np.float64(THETA), -half.astype(np.float64)).astype(np.float32)
    freq = np.concatenate([freq, freq])[None, :]

    def per_device(q_raw, k_raw, v_raw, positions, seq_ids, q_gain, k_gain):
        vmem = pl.BlockSpec(memory_space=pltpu.VMEM)
        hbm = pl.BlockSpec(memory_space=pltpu.HBM)
        sem = pltpu.SemaphoreType.DMA((CHIPS, PARTS))
        inputs = (q_raw, k_raw, v_raw, positions[None, :], seq_ids[None, :], q_gain[None, :], k_gain[None, :], jnp.asarray(freq))
        out, lse = pl.pallas_call(
            kernel,
            out_shape=(jax.ShapeDtypeStruct((QH, T, D), BF16), jax.ShapeDtypeStruct((QH, T), F32)),
            in_specs=[hbm] * 8,
            out_specs=(vmem, vmem),
            scratch_shapes=[
                pltpu.VMEM((CHIPS, 2, KVH, 2, 2, HALF, D), BF16),
                pltpu.VMEM((3, KVH, D, GROUP * HALF), BF16),
                pltpu.VMEM((3, KVH, D, GROUP * HALF), F32),
                pltpu.VMEM((3, KVH, 1, GROUP * HALF), F32),
                pltpu.VMEM((3, KVH, 1, GROUP * HALF), F32),
                pltpu.VMEM((3, 2 * HALF, HALF), F32),
                pltpu.VMEM((2, T, D), F32),
                pltpu.VMEM((T, T), BF16),
                pltpu.VMEM((T, QH, D), BF16),
                pltpu.VMEM((T, KVH, D), BF16),
                pltpu.VMEM((T, KVH, D), BF16),
                pltpu.VMEM((1, T), jnp.int32),
                pltpu.VMEM((1, T), jnp.int32),
                pltpu.VMEM((1, D), BF16),
                pltpu.VMEM((1, D), BF16),
                pltpu.VMEM((1, D), F32),
                sem, sem, sem, sem, sem, sem,
                pltpu.SemaphoreType.DMA((8,)),
                pltpu.SemaphoreType.DMA((3,)),
                pltpu.SemaphoreType.DMA((3,)),
                pltpu.VMEM((T, T), BF16),
                pltpu.VMEM((KVH, 1, 2 * GROUP * HALF), F32),
                pltpu.VMEM((D, GROUP * HALF), BF16),
                pltpu.VMEM((1, GROUP * HALF), F32),
            ],
            compiler_params=pltpu.CompilerParams(collective_id=0, has_side_effects=True, vmem_limit_bytes=48 * 1024 * 1024),
            name="gather_attend",
        )(*[pltpu.with_memory_space_constraint(x, pltpu.HBM) for x in inputs])
        return jnp.transpose(out, (1, 0, 2)), lse.T

    return jax.shard_map(per_device, mesh=mesh, in_specs=(P("cp", "tp", None), P("cp", "tp", None), P("cp", "tp", None), P("cp"), P("cp"), P(), P()), out_specs=(P("cp", "tp", None), P("cp", "tp")), check_vma=False)
```

```python
import functools
import math

import jax
import jax.numpy as jnp
import numpy as np
from jax import lax
from jax.experimental import pallas as pl
from jax.experimental.pallas import tpu as pltpu
from jax.sharding import PartitionSpec as P

THETA = 1000000.0
EPS = 1e-6
NEG = -1e30
LAYERS = 4
CHIPS = 8
CP = 16
T = 256
HALF = 128
KVH = 4
GROUP = 4
QH = KVH * GROUP
D = 128
LOG2E = math.log2(math.e)
LN2 = math.log(2.0)
SCALE2 = D ** -0.5 * LOG2E
EVENTS = (
    (0x12084140, 0x0a501009, 0x18481a0b, 0x222a5820, 0x68322860, 0x3a703038, 0xff858478, 0xffffffff, 0xffffffff, 0xffffffff, 0xffffffff, 0xffffffff, 0xffffffff, 0xffffffff),
    (0x1a490148, 0x18400041, 0x102a1258, 0x38682850, 0x78223a20, 0x70303260, 0xffff8584, 0xffffffff, 0xffffffff, 0xffffffff, 0xffffffff, 0xffffffff, 0xffffffff, 0xffffffff),
    (0x231b0151, 0x00412150, 0x0320611a, 0x90821840, 0x58a01922, 0x59330831, 0x7198092a, 0x49b00b29, 0x48882b32, 0x3028a869, 0x38683b60, 0xb8797039, 0x7885813a, 0xffffff84),
    (0x10085859, 0x2911092a, 0x2b130b48, 0x23514901, 0x2128908a, 0x61804198, 0x003869a0, 0x3a4050a8, 0x393b6820, 0x31792278, 0x336030b8, 0x3281b071, 0xff847085, 0xffffffff),
    (0x10333160, 0x1150612a, 0x2b320129, 0x69514171, 0x68003028, 0x1838403b, 0x08581970, 0x09483a59, 0x79497839, 0xffff8584, 0xffffffff, 0xffffffff, 0xffffffff, 0xffffffff),
    (0x18692168, 0x19206138, 0x333a3158, 0x083b6059, 0x10097139, 0x49110148, 0x32504130, 0x00707851, 0x84408579, 0xffffffff, 0xffffffff, 0xffffffff, 0xffffffff, 0xffffffff),
    (0x38712170, 0x3a602061, 0x3978103b, 0x01295011, 0x79416951, 0x68190028, 0x58185940, 0x84094808, 0xffff8549, 0xffffffff, 0xffffffff, 0xffffffff, 0xffffffff, 0xffffffff),
    (0x79312978, 0x71302869, 0x70616821, 0x58192018, 0x11106059, 0x48095108, 0x00504901, 0x84408541, 0xffffffff, 0xffffffff, 0xffffffff, 0xffffffff, 0xffffffff, 0xffffffff),
)
ROUTES = (
    (0x5824f836, 0x50005082, 0x50005082, 0x50005080),
    (0xfcb63000, 0x50025000, 0x50825000, 0x50825000),
    (0xb024b036, 0xf044f477, 0xf000f4d3, 0xf000f4d1),
    (0xb0243020, 0xf4f7b000, 0xf4d3f000, 0xf0c3f001),
    (0x30243026, 0x30043036, 0xf000f27f, 0xf208f6d9),
    (0x30243020, 0x30343000, 0xf6ff3020, 0xf2dbf001),
    (0x30003002, 0x30003012, 0x30003002, 0xf200f25b),
    (0x30003000, 0x30103000, 0x30123000, 0xf6db3001),
)
FIRST = (0x60a, 0x688, 0x642, 0x213, 0x40b, 0x0ca, 0x099, 0x2d0)
GUEST = 2
BITS = 8
PER_WORD = 4
WORDS = len(EVENTS[0])
PARTS = 4
GROUPS = ((0, 1, 2), (3,))


def signed(word):
    return word - (1 << 32) if word >= 1 << 31 else word


def select(index, values):
    values = [jnp.int32(v) if isinstance(v, int) else v for v in values]
    while len(values) > 1:
        odd = index % 2 == 1
        values = [jnp.where(odd, values[i + 1], values[i]) if i + 1 < len(values) else values[i] for i in range(0, len(values), 2)]
        index = index // 2
    return values[0]


E, L = 0, 1
F32 = jnp.float32
BF16 = jnp.bfloat16
MESH = pl.DeviceIdType.MESH


def dot(a, b, dims, precision=None):
    return lax.dot_general(a, b, (dims, ((), ())), preferred_element_type=F32, precision=precision)


def column(row, ident):
    return jnp.sum(jnp.where(ident, row, 0.0), axis=1, keepdims=True)


def norm_rope(x, gain, cos, sin):
    inv = lax.rsqrt(jnp.mean(x * x, axis=-1, keepdims=True) + EPS)
    normed = (x * inv * gain).astype(BF16).astype(F32)
    return (normed * cos + pltpu.roll(normed, D // 2, 1) * sin).astype(BF16)


def kernel(q_hbm, k_hbm, v_hbm, pos_hbm, seq_hbm, qg_hbm, kg_hbm, freq_hbm, o_ref, lse_ref,
           kvbuf, qbuf, acc, mst, lst, bias, rope, perm,
           q_in, k_in, v_in, pos_ref, seq_ref, qg_ref, kg_ref, freq_ref,
           s_dn, s_up, s_y, s_d, r_link, r_d, s_in, s_x, r_x,
           perm_t, logs, x_out, x_log):
    me = lax.axis_index("cp")
    z = me // 4
    y = (me // 2) % 2
    c = me % 2
    own = me // 2

    def dev(zz, yy, cc):
        return {"cp": zz * 4 + yy * 2 + cc}

    barrier = pltpu.get_barrier_semaphore()
    pl.semaphore_signal(barrier, inc=1, device_id=dev(z, y, 1 - c), device_id_type=MESH)
    pl.semaphore_signal(barrier, inc=1, device_id=dev(z, 1 - y, c), device_id_type=MESH)

    @pl.when(z > 0)
    def _():
        pl.semaphore_signal(barrier, inc=1, device_id=dev(z - 1, y, c), device_id_type=MESH)

    @pl.when(z < LAYERS - 1)
    def _():
        pl.semaphore_signal(barrier, inc=1, device_id=dev(z + 1, y, c), device_id_type=MESH)

    pairs = ((pos_hbm, pos_ref), (seq_hbm, seq_ref), (freq_hbm, freq_ref), (kg_hbm, kg_ref), (k_hbm, k_in), (v_hbm, v_in),
             (qg_hbm, qg_ref), (q_hbm, q_in))
    loads = [pltpu.make_async_copy(src, dst, s_in.at[i]) for i, (src, dst) in enumerate(pairs)]
    for load in loads:
        load.start()
    loads[0].wait()
    loads[1].wait()

    row_i = lax.broadcasted_iota(jnp.int32, (T, T), 0)
    col_i = lax.broadcasted_iota(jnp.int32, (T, T), 1)
    ident = row_i == col_i
    pos_row = pos_ref[...].astype(F32)
    seq_row = seq_ref[...].astype(F32)
    pos_col = column(pos_row, ident)
    seq_col = column(seq_row, ident)
    same = (seq_col == seq_row).astype(F32)
    early_row = (pos_row < 8.0 * jnp.sum(same, axis=0, keepdims=True)).astype(F32)
    early_col = (pos_col < 8.0 * jnp.sum(same, axis=1, keepdims=True)).astype(F32)
    alike = (early_col == early_row).astype(F32)
    dest_row = jnp.sum(jnp.where(row_i < col_i, alike, 0.0), axis=0, keepdims=True) + HALF * (1.0 - early_row)
    one_hot = (row_i.astype(F32) == dest_row).astype(BF16)
    perm[...] = one_hot

    left = lax.broadcasted_iota(jnp.int32, (HALF, D), 1) < D // 2
    loads[2].wait()
    angle = jnp.where(left, pos_col[:HALF], pos_col[HALF:]) * freq_ref[...]
    cos = jnp.cos(angle)
    sin = jnp.sin(angle)
    cos_r = pltpu.roll(cos, D // 2, 1)
    sin_r = pltpu.roll(sin, D // 2, 1)
    cos = jnp.concatenate([jnp.where(left, cos, cos_r), jnp.where(left, cos_r, cos)], axis=0)
    sin = jnp.concatenate([jnp.where(left, -sin, sin_r), jnp.where(left, -sin_r, sin)], axis=0)
    rope[0] = cos
    rope[1] = sin

    loads[3].wait()
    loads[4].wait()
    loads[5].wait()
    k_all = jnp.transpose(k_in[...].astype(F32), (1, 0, 2))
    v_all = jnp.transpose(v_in[...].astype(F32), (1, 0, 2)).astype(BF16)
    gain = kg_ref[...].astype(F32)
    for h in range(KVH):
        kr = dot(one_hot, norm_rope(k_all[h], gain, cos, sin), ((1,), (0,))).astype(BF16)
        vr = dot(v_all[h], one_hot, ((0,), (1,))).astype(BF16)
        for part in (E, L):
            kvbuf[own, part, h, 0, c] = kr[part * HALF:(part + 1) * HALF]
            kvbuf[own, part, h, 1, c] = vr[:, part * HALF:(part + 1) * HALF]

    pl.semaphore_wait(barrier, 2 + jnp.minimum(z, 1) + jnp.minimum(LAYERS - 1 - z, 1))

    class Copy:
        def __init__(self, m, part, send, recv, target):
            self.args = (m, part, send, recv, target)

        def act(self, name):
            m, part, send, recv, target = self.args

            def run(g):
                ref = kvbuf.at[m, part // 2, pl.ds(GROUPS[g][0], len(GROUPS[g])), :, c]
                getattr(pltpu.make_async_remote_copy(
                    src_ref=ref, dst_ref=ref, send_sem=send.at[m, part], recv_sem=recv.at[m, part],
                    device_id=target, device_id_type=MESH), name)()

            if isinstance(part, int):
                run(part % 2)
            else:
                pl.when(part % 2 == 0)(lambda: run(0))
                pl.when(part % 2 == 1)(lambda: run(1))

        def start(self):
            self.act("start")

        def wait_recv(self):
            self.act("wait_recv")

        def wait_send(self):
            self.act("wait_send")

    def down(m, part):
        return Copy(m, part, s_dn, r_link, dev(z - 1, y, c))

    def up(m, part):
        return Copy(m, part, s_up, r_link, dev(z + 1, y, c))

    def across(m, part):
        return Copy(m, part, s_y, r_link, dev(z, 1 - y, c))

    def partner(m, part):
        return Copy(m, part, s_d, r_d, dev(z, y, 1 - c))

    route_words = [select(own, [signed(row[pair]) for row in ROUTES]) for pair in range(CHIPS // 2)]
    event_words = [select(own, [signed(row[w]) for row in EVENTS]) for w in range(WORDS)]
    first_word = select(own, list(FIRST))

    def routes(m, part):
        entry = jnp.right_shift(select(m // 2, route_words), 16 * (m % 2))
        way = jnp.right_shift(entry, 3 * part) % 8
        need = jnp.right_shift(entry, 3 * PARTS + part) % 2
        return way % 2 == 1, (way // 2) % 2 == 1, way // 4 == 1, need == 1

    def forward(m, part):
        go_down, go_across, go_up, go_partner = routes(m, part)

        @pl.when(go_down)
        def _():
            down(m, part).start()

        @pl.when(go_across)
        def _():
            across(m, part).start()

        @pl.when(go_up)
        def _():
            up(m, part).start()

        @pl.when(go_partner)
        def _():
            partner(m, part).start()

    @pl.loop(0, PARTS)
    def _(i):
        forward(own, jnp.right_shift(first_word, 3 * i) % 8)

    loads[6].wait()
    loads[7].wait()
    q_all = jnp.transpose(q_in[...].astype(F32), (1, 0, 2))
    q_gain = qg_ref[...].astype(F32)
    for h in range(QH):
        qr = dot(norm_rope(q_all[h], q_gain, rope[0], rope[1]), perm[...], ((0,), (1,))).astype(BF16)
        for part in (E, L):
            qbuf[part, h // GROUP, :, (h % GROUP) * HALF:(h % GROUP + 1) * HALF] = qr[:, part * HALF:(part + 1) * HALF]

    def ship(i, src, dst, zz):
        return pltpu.make_async_remote_copy(
            src_ref=src, dst_ref=dst, send_sem=s_x.at[i], recv_sem=r_x.at[i], device_id=dev(zz, y, c), device_id_type=MESH)

    def ship_queries():
        return ship(0, qbuf.at[L, KVH - 1], qbuf.at[GUEST, KVH - 1], 1 - z)

    def ship_results():
        return ship(1, x_out, x_out, 1 - z), ship(2, x_log, x_log, 1 - z)

    seg = dot(perm[0:HALF], same.astype(BF16), ((1,), (0,))).astype(BF16)
    seg = dot(seg, perm[0:HALF], ((1,), (1,))) > 0.5
    r_i = lax.broadcasted_iota(jnp.int32, (HALF, HALF), 0)
    c_i = lax.broadcasted_iota(jnp.int32, (HALF, HALF), 1)
    full = jnp.where(seg, 0.0, NEG)
    diag = jnp.where(jnp.logical_and(seg, r_i <= c_i), 0.0, NEG)
    none = jnp.full((HALF, HALF), NEG, F32)
    first = c == 0
    bias[0, 0:HALF] = full
    bias[0, HALF:] = full
    bias[1, 0:HALF] = jnp.where(first, diag, full)
    bias[1, HALF:] = jnp.where(first, none, diag)
    bias[2, 0:HALF] = jnp.where(first, diag, none)
    bias[2, HALF:] = jnp.where(first, full, diag)

    @pl.when(z == 0)
    def _():
        ship_queries().start()

    mst[...] = jnp.full(mst.shape, NEG, F32)
    lst[...] = jnp.zeros(lst.shape, F32)
    acc[...] = jnp.zeros(acc.shape, F32)

    def attend(m, heads, groups):
        work = [(h, qp, keys) for h in heads for qp, keys in groups]
        scores = []
        for h, qp, keys in work:
            q = qbuf[qp, h]
            scores.append([dot(kvbuf[m, piece, h, 0].reshape(2 * HALF, D), q, ((1,), (0,))) for piece, _ in keys])
        for (h, qp, keys), group in zip(work, scores):
            group = [s * SCALE2 + jnp.concatenate([bias[b]] * GROUP, axis=1) for s, (_, b) in zip(group, keys)]
            m_old = mst[qp, h]
            m_new = m_old
            for s in group:
                m_new = jnp.maximum(m_new, jnp.max(s, axis=0, keepdims=True))
            alpha = jnp.exp2(m_old - m_new)
            total = lst[qp, h] * alpha
            out = acc[qp, h] * alpha
            for s, (piece, _) in zip(group, keys):
                p = jnp.exp2(s - m_new)
                total = total + jnp.sum(p, axis=0, keepdims=True)
                vals = kvbuf[m, piece, h, 1]
                out = out + dot(jnp.concatenate([vals[0], vals[1]], axis=1), p.astype(BF16), ((1,), (0,)))
            mst[qp, h] = m_new
            lst[qp, h] = total
            acc[qp, h] = out

    back = jnp.transpose(perm[...].astype(F32), (1, 0)).astype(BF16)
    perm_t[...] = back

    def finish(h):
        outs = []
        for part in (E, L):
            total = lst[part, h]
            out = (acc[part, h] / total).astype(BF16)
            log = mst[part, h] * LN2 + jnp.log(total)
            outs.append(out)
            logs[h, :, part * GROUP * HALF:(part + 1) * GROUP * HALF] = log
        for g in range(0, GROUP, 2):
            stack = []
            for i in (g, g + 1):
                cols = slice(i * HALF, (i + 1) * HALF)
                stack.append(jnp.concatenate([outs[0][:, cols], outs[1][:, cols]], axis=1))
            two = dot(perm_t[...], jnp.concatenate(stack, axis=0), ((1,), (1,))).astype(BF16)
            o_ref[h * GROUP + g] = two[:, 0:D]
            o_ref[h * GROUP + g + 1] = two[:, D:]

    def step(event):
        kind = event // 64
        m = (event // 8) % CHIPS
        low = event % 8

        @pl.when(kind == 0)
        def _():
            across(m, low).wait_recv()
            forward(m, low)

        for g, heads in enumerate(GROUPS):
            @pl.when(jnp.logical_and(kind == 1, low == g))
            def _():
                partner(m, g).wait_recv()

                @pl.when(m >= own)
                def _():
                    partner(m, 2 + g).wait_recv()

                away = z == 0 if g == 1 else z < 0
                here = jnp.logical_not(away)

                @pl.when(jnp.logical_and(here, m > own))
                def _():
                    attend(m, heads, [(L, [(E, 0), (L, 0)])])

                @pl.when(jnp.logical_and(here, m < own))
                def _():
                    attend(m, heads, [(E, [(E, 0)]), (L, [(E, 0)])])

                @pl.when(jnp.logical_and(here, m == own))
                def _():
                    attend(m, heads, [(E, [(E, 1)]), (L, [(L, 2), (E, 0)])])

                if g == 1:
                    @pl.when(away)
                    def _():
                        attend(m, heads, [(E, [(E, jnp.where(m == own, 1, 0))])])

        @pl.when(jnp.logical_and(kind == 2, jnp.logical_or(low == 0, low == 2)))
        def _():
            @pl.when(low == 2)
            def _():
                ship_queries().wait_recv()

            @pl.when(jnp.logical_and(m >= y, m < own))
            def _():
                partner(m, PARTS - 1).wait_recv()

            @pl.when(m >= y)
            def _():
                attend(m, GROUPS[1], [(GUEST, [(E, 0), (L, jnp.where(m == y, 2, 0))])])

            @pl.when(m < y)
            def _():
                attend(m, GROUPS[1], [(GUEST, [(E, 0)])])

        @pl.when(jnp.logical_and(kind == 2, low == 1))
        def _():
            total = lst[GUEST, KVH - 1]
            x_out[...] = (acc[GUEST, KVH - 1] / total).astype(BF16)
            x_log[...] = mst[GUEST, KVH - 1] * LN2 + jnp.log(total)
            for x in ship_results():
                x.start()

        @pl.when(jnp.logical_and(kind == 2, low == 4))
        def _():
            for h in GROUPS[0]:
                finish(h)

        @pl.when(jnp.logical_and(kind == 2, low == 5))
        def _():
            @pl.when(z == 0)
            def _():
                for x in ship_results():
                    x.wait_recv()
                acc[L, KVH - 1] = x_out[...].astype(F32)
                lst[L, KVH - 1] = jnp.ones((1, GROUP * HALF), F32)
                mst[L, KVH - 1] = x_log[...] * LOG2E

            finish(KVH - 1)

    @pl.loop(0, WORDS)
    def _(n):
        word = select(n, event_words)

        @pl.loop(0, PER_WORD)
        def _(i):
            step(jnp.right_shift(word, BITS * i) % (1 << BITS))

    lse = []
    for part in (E, L):
        rows = []
        for h in range(KVH):
            for g in range(GROUP):
                at = (part * GROUP + g) * HALF
                rows.append(logs[h, :, at:at + HALF])
        lse.append(jnp.concatenate(rows, axis=0))
    lse = jnp.concatenate(lse, axis=1)
    lse_ref[...] = dot(lse, perm[...].astype(F32), ((1,), (0,)), precision=lax.Precision.HIGHEST)

    @pl.loop(0, CHIPS * PARTS)
    def _(i):
        m = i // PARTS
        part = i % PARTS
        go_down, go_across, go_up, go_partner = routes(m, part)

        @pl.when(go_partner)
        def _():
            partner(m, part).wait_send()

        @pl.when(go_down)
        def _():
            down(m, part).wait_send()

        @pl.when(go_across)
        def _():
            across(m, part).wait_send()

        @pl.when(go_up)
        def _():
            up(m, part).wait_send()

    @pl.when(z == 0)
    def _():
        ship_queries().wait_send()

    @pl.when(z == 1)
    def _():
        for x in ship_results():
            x.wait_send()


def solution(mesh):
    half = np.arange(D // 2, dtype=np.float32) * np.float32(2.0) / np.float32(D)
    freq = np.power(np.float64(THETA), -half.astype(np.float64)).astype(np.float32)
    freq = np.concatenate([freq, freq])[None, :]

    def per_device(q_raw, k_raw, v_raw, positions, seq_ids, q_gain, k_gain):
        vmem = pl.BlockSpec(memory_space=pltpu.VMEM)
        hbm = pl.BlockSpec(memory_space=pltpu.HBM)
        sem = pltpu.SemaphoreType.DMA((CHIPS, PARTS))
        inputs = (q_raw, k_raw, v_raw, positions[None, :], seq_ids[None, :], q_gain[None, :], k_gain[None, :], jnp.asarray(freq))
        out, lse = pl.pallas_call(
            kernel,
            out_shape=(jax.ShapeDtypeStruct((QH, T, D), BF16), jax.ShapeDtypeStruct((QH, T), F32)),
            in_specs=[hbm] * 8,
            out_specs=(vmem, vmem),
            scratch_shapes=[
                pltpu.VMEM((CHIPS, 2, KVH, 2, 2, HALF, D), BF16),
                pltpu.VMEM((3, KVH, D, GROUP * HALF), BF16),
                pltpu.VMEM((3, KVH, D, GROUP * HALF), F32),
                pltpu.VMEM((3, KVH, 1, GROUP * HALF), F32),
                pltpu.VMEM((3, KVH, 1, GROUP * HALF), F32),
                pltpu.VMEM((3, 2 * HALF, HALF), F32),
                pltpu.VMEM((2, T, D), F32),
                pltpu.VMEM((T, T), BF16),
                pltpu.VMEM((T, QH, D), BF16),
                pltpu.VMEM((T, KVH, D), BF16),
                pltpu.VMEM((T, KVH, D), BF16),
                pltpu.VMEM((1, T), jnp.int32),
                pltpu.VMEM((1, T), jnp.int32),
                pltpu.VMEM((1, D), BF16),
                pltpu.VMEM((1, D), BF16),
                pltpu.VMEM((1, D), F32),
                sem, sem, sem, sem, sem, sem,
                pltpu.SemaphoreType.DMA((8,)),
                pltpu.SemaphoreType.DMA((3,)),
                pltpu.SemaphoreType.DMA((3,)),
                pltpu.VMEM((T, T), BF16),
                pltpu.VMEM((KVH, 1, 2 * GROUP * HALF), F32),
                pltpu.VMEM((D, GROUP * HALF), BF16),
                pltpu.VMEM((1, GROUP * HALF), F32),
            ],
            compiler_params=pltpu.CompilerParams(collective_id=0, has_side_effects=True, vmem_limit_bytes=48 * 1024 * 1024),
            name="gather_attend",
        )(*[pltpu.with_memory_space_constraint(x, pltpu.HBM) for x in inputs])
        return jnp.transpose(out, (1, 0, 2)), lse.T

    return jax.shard_map(per_device, mesh=mesh, in_specs=(P("cp", "tp", None), P("cp", "tp", None), P("cp", "tp", None), P("cp"), P("cp"), P(), P()), out_specs=(P("cp", "tp", None), P("cp", "tp")), check_vma=False)
```

```python
import functools
import math

import jax
import jax.numpy as jnp
import numpy as np
from jax import lax
from jax.experimental import pallas as pl
from jax.experimental.pallas import tpu as pltpu
from jax.sharding import PartitionSpec as P

THETA = 1000000.0
EPS = 1e-6
NEG = -1e30
LAYERS = 4
CHIPS = 8
CP = 16
T = 256
HALF = 128
KVH = 4
GROUP = 4
QH = KVH * GROUP
D = 128
LOG2E = math.log2(math.e)
LN2 = math.log(2.0)
SCALE2 = D ** -0.5 * LOG2E
EVENTS = (
    (0x12084140, 0x0a501009, 0x18481a0b, 0x222a5820, 0x68322860, 0x3a703038, 0xff858478, 0xffffffff, 0xffffffff, 0xffffffff, 0xffffffff, 0xffffffff, 0xffffffff, 0xffffffff),
    (0x1a490148, 0x18400041, 0x102a1258, 0x38682850, 0x78223a20, 0x70303260, 0xffff8584, 0xffffffff, 0xffffffff, 0xffffffff, 0xffffffff, 0xffffffff, 0xffffffff, 0xffffffff),
    (0x231b0151, 0x00412150, 0x0320611a, 0x90821840, 0x58a01922, 0x59330831, 0x7198092a, 0x49b00b29, 0x48882b32, 0x3028a869, 0x38683b60, 0xb8797039, 0x7885813a, 0xffffff84),
    (0x10085859, 0x2911092a, 0x2b130b48, 0x23514901, 0x2128908a, 0x61804198, 0x003869a0, 0x3a4050a8, 0x393b6820, 0x31792278, 0x336030b8, 0x3281b071, 0xff847085, 0xffffffff),
    (0x10333160, 0x1150612a, 0x2b320129, 0x69514171, 0x68003028, 0x1838403b, 0x08581970, 0x09483a59, 0x79497839, 0xffff8584, 0xffffffff, 0xffffffff, 0xffffffff, 0xffffffff),
    (0x18692168, 0x19206138, 0x333a3158, 0x083b6059, 0x10097139, 0x49110148, 0x32504130, 0x00707851, 0x84408579, 0xffffffff, 0xffffffff, 0xffffffff, 0xffffffff, 0xffffffff),
    (0x38712170, 0x3a602061, 0x3978103b, 0x01295011, 0x79416951, 0x68190028, 0x58185940, 0x84094808, 0xffff8549, 0xffffffff, 0xffffffff, 0xffffffff, 0xffffffff, 0xffffffff),
    (0x79312978, 0x71302869, 0x70616821, 0x58192018, 0x11106059, 0x48095108, 0x00504901, 0x84408541, 0xffffffff, 0xffffffff, 0xffffffff, 0xffffffff, 0xffffffff, 0xffffffff),
)
ROUTES = (
    (0x5824f836, 0x50005082, 0x50005082, 0x50005080),
    (0xfcb63000, 0x50025000, 0x50825000, 0x50825000),
    (0xb024b036, 0xf044f477, 0xf000f4d3, 0xf000f4d1),
    (0xb0243020, 0xf4f7b000, 0xf4d3f000, 0xf0c3f001),
    (0x30243026, 0x30043036, 0xf000f27f, 0xf208f6d9),
    (0x30243020, 0x30343000, 0xf6ff3020, 0xf2dbf001),
    (0x30003002, 0x30003012, 0x30003002, 0xf200f25b),
    (0x30003000, 0x30103000, 0x30123000, 0xf6db3001),
)
FIRST = (0x60a, 0x688, 0x642, 0x213, 0x40b, 0x0ca, 0x099, 0x2d0)
GUEST = 2
BITS = 8
PER_WORD = 4
WORDS = len(EVENTS[0])
PARTS = 4
GROUPS = ((0, 1, 2), (3,))


def signed(word):
    return word - (1 << 32) if word >= 1 << 31 else word


def select(index, values):
    values = [jnp.int32(v) if isinstance(v, int) else v for v in values]
    while len(values) > 1:
        odd = index % 2 == 1
        values = [jnp.where(odd, values[i + 1], values[i]) if i + 1 < len(values) else values[i] for i in range(0, len(values), 2)]
        index = index // 2
    return values[0]


E, L = 0, 1
F32 = jnp.float32
BF16 = jnp.bfloat16
MESH = pl.DeviceIdType.MESH


def dot(a, b, dims, precision=None):
    return lax.dot_general(a, b, (dims, ((), ())), preferred_element_type=F32, precision=precision)


def column(row, ident):
    return jnp.sum(jnp.where(ident, row, 0.0), axis=1, keepdims=True)


def norm_rope(x, gain, cos, sin):
    inv = lax.rsqrt(jnp.mean(x * x, axis=-1, keepdims=True) + EPS)
    normed = (x * inv * gain).astype(BF16).astype(F32)
    return (normed * cos + pltpu.roll(normed, D // 2, 1) * sin).astype(BF16)


def kernel(q_hbm, k_hbm, v_hbm, pos_hbm, seq_hbm, qg_hbm, kg_hbm, freq_hbm, o_ref, lse_ref,
           kvbuf, qbuf, acc, mst, lst, bias, rope, perm,
           q_in, k_in, v_in, pos_ref, seq_ref, qg_ref, kg_ref, freq_ref,
           s_dn, s_up, s_y, s_d, r_link, r_d, s_in, s_x, r_x,
           perm_t, logs, x_out, x_log):
    me = lax.axis_index("cp")
    z = me // 4
    y = (me // 2) % 2
    c = me % 2
    own = me // 2

    def dev(zz, yy, cc):
        return {"cp": zz * 4 + yy * 2 + cc}

    barrier = pltpu.get_barrier_semaphore()
    pl.semaphore_signal(barrier, inc=1, device_id=dev(z, y, 1 - c), device_id_type=MESH)
    pl.semaphore_signal(barrier, inc=1, device_id=dev(z, 1 - y, c), device_id_type=MESH)

    @pl.when(z > 0)
    def _():
        pl.semaphore_signal(barrier, inc=1, device_id=dev(z - 1, y, c), device_id_type=MESH)

    @pl.when(z < LAYERS - 1)
    def _():
        pl.semaphore_signal(barrier, inc=1, device_id=dev(z + 1, y, c), device_id_type=MESH)

    pairs = ((pos_hbm, pos_ref), (seq_hbm, seq_ref), (freq_hbm, freq_ref), (kg_hbm, kg_ref), (k_hbm, k_in), (v_hbm, v_in),
             (qg_hbm, qg_ref), (q_hbm, q_in))
    loads = [pltpu.make_async_copy(src, dst, s_in.at[i]) for i, (src, dst) in enumerate(pairs)]
    for load in loads:
        load.start()
    loads[0].wait()
    loads[1].wait()

    row_i = lax.broadcasted_iota(jnp.int32, (T, T), 0)
    col_i = lax.broadcasted_iota(jnp.int32, (T, T), 1)
    ident = row_i == col_i
    pos_row = pos_ref[...].astype(F32)
    seq_row = seq_ref[...].astype(F32)
    pos_col = column(pos_row, ident)
    seq_col = column(seq_row, ident)
    same = (seq_col == seq_row).astype(F32)
    early_row = (pos_row < 8.0 * jnp.sum(same, axis=0, keepdims=True)).astype(F32)
    early_col = (pos_col < 8.0 * jnp.sum(same, axis=1, keepdims=True)).astype(F32)
    alike = (early_col == early_row).astype(F32)
    dest_row = jnp.sum(jnp.where(row_i < col_i, alike, 0.0), axis=0, keepdims=True) + HALF * (1.0 - early_row)
    one_hot = (row_i.astype(F32) == dest_row).astype(BF16)
    perm[...] = one_hot

    left = lax.broadcasted_iota(jnp.int32, (HALF, D), 1) < D // 2
    loads[2].wait()
    angle = jnp.where(left, pos_col[:HALF], pos_col[HALF:]) * freq_ref[...]
    cos = jnp.cos(angle)
    sin = jnp.sin(angle)
    cos_r = pltpu.roll(cos, D // 2, 1)
    sin_r = pltpu.roll(sin, D // 2, 1)
    cos = jnp.concatenate([jnp.where(left, cos, cos_r), jnp.where(left, cos_r, cos)], axis=0)
    sin = jnp.concatenate([jnp.where(left, -sin, sin_r), jnp.where(left, -sin_r, sin)], axis=0)
    rope[0] = cos
    rope[1] = sin

    loads[3].wait()
    loads[4].wait()
    loads[5].wait()
    k_all = jnp.transpose(k_in[...].astype(F32), (1, 0, 2))
    v_all = jnp.transpose(v_in[...].astype(F32), (1, 0, 2)).astype(BF16)
    gain = kg_ref[...].astype(F32)
    for h in range(KVH):
        kr = dot(one_hot, norm_rope(k_all[h], gain, cos, sin), ((1,), (0,))).astype(BF16)
        vr = dot(v_all[h], one_hot, ((0,), (1,))).astype(BF16)
        for part in (E, L):
            kvbuf[own, part, h, 0, c] = kr[part * HALF:(part + 1) * HALF]
            kvbuf[own, part, h, 1, c] = vr[:, part * HALF:(part + 1) * HALF]

    pl.semaphore_wait(barrier, 2 + jnp.minimum(z, 1) + jnp.minimum(LAYERS - 1 - z, 1))

    class Copy:
        def __init__(self, m, part, send, recv, target):
            self.args = (m, part, send, recv, target)

        def act(self, name):
            m, part, send, recv, target = self.args

            def run(g):
                ref = kvbuf.at[m, part // 2, pl.ds(GROUPS[g][0], len(GROUPS[g])), :, c]
                getattr(pltpu.make_async_remote_copy(
                    src_ref=ref, dst_ref=ref, send_sem=send.at[m, part], recv_sem=recv.at[m, part],
                    device_id=target, device_id_type=MESH), name)()

            if isinstance(part, int):
                run(part % 2)
            else:
                pl.when(part % 2 == 0)(lambda: run(0))
                pl.when(part % 2 == 1)(lambda: run(1))

        def start(self):
            self.act("start")

        def wait_recv(self):
            self.act("wait_recv")

        def wait_send(self):
            self.act("wait_send")

    def down(m, part):
        return Copy(m, part, s_dn, r_link, dev(z - 1, y, c))

    def up(m, part):
        return Copy(m, part, s_up, r_link, dev(z + 1, y, c))

    def across(m, part):
        return Copy(m, part, s_y, r_link, dev(z, 1 - y, c))

    def partner(m, part):
        return Copy(m, part, s_d, r_d, dev(z, y, 1 - c))

    route_words = [select(own, [signed(row[pair]) for row in ROUTES]) for pair in range(CHIPS // 2)]
    event_words = [select(own, [signed(row[w]) for row in EVENTS]) for w in range(WORDS)]
    first_word = select(own, list(FIRST))

    def routes(m, part):
        entry = jnp.right_shift(select(m // 2, route_words), 16 * (m % 2))
        way = jnp.right_shift(entry, 3 * part) % 8
        need = jnp.right_shift(entry, 3 * PARTS + part) % 2
        return way % 2 == 1, (way // 2) % 2 == 1, way // 4 == 1, need == 1

    def forward(m, part):
        go_down, go_across, go_up, go_partner = routes(m, part)

        @pl.when(go_down)
        def _():
            down(m, part).start()

        @pl.when(go_across)
        def _():
            across(m, part).start()

        @pl.when(go_up)
        def _():
            up(m, part).start()

        @pl.when(go_partner)
        def _():
            partner(m, part).start()

    @pl.loop(0, PARTS)
    def _(i):
        forward(own, jnp.right_shift(first_word, 3 * i) % 8)

    loads[6].wait()
    loads[7].wait()
    q_all = jnp.transpose(q_in[...].astype(F32), (1, 0, 2))
    q_gain = qg_ref[...].astype(F32)
    for h in range(QH):
        qr = dot(norm_rope(q_all[h], q_gain, rope[0], rope[1]), perm[...], ((0,), (1,))).astype(BF16)
        for part in (E, L):
            qbuf[part, h // GROUP, :, (h % GROUP) * HALF:(h % GROUP + 1) * HALF] = qr[:, part * HALF:(part + 1) * HALF]

    def ship(i, src, dst, zz):
        return pltpu.make_async_remote_copy(
            src_ref=src, dst_ref=dst, send_sem=s_x.at[i], recv_sem=r_x.at[i], device_id=dev(zz, y, c), device_id_type=MESH)

    def ship_queries():
        return ship(0, qbuf.at[L, KVH - 1], qbuf.at[GUEST, KVH - 1], 1 - z)

    def ship_results():
        return ship(1, x_out, x_out, 1 - z), ship(2, x_log, x_log, 1 - z)

    seg = dot(perm[0:HALF], same.astype(BF16), ((1,), (0,))).astype(BF16)
    seg = dot(seg, perm[0:HALF], ((1,), (1,))) > 0.5
    r_i = lax.broadcasted_iota(jnp.int32, (HALF, HALF), 0)
    c_i = lax.broadcasted_iota(jnp.int32, (HALF, HALF), 1)
    full = jnp.where(seg, 0.0, NEG)
    diag = jnp.where(jnp.logical_and(seg, r_i <= c_i), 0.0, NEG)
    none = jnp.full((HALF, HALF), NEG, F32)
    first = c == 0
    bias[0, 0:HALF] = full
    bias[0, HALF:] = full
    bias[1, 0:HALF] = jnp.where(first, diag, full)
    bias[1, HALF:] = jnp.where(first, none, diag)
    bias[2, 0:HALF] = jnp.where(first, diag, none)
    bias[2, HALF:] = jnp.where(first, full, diag)

    @pl.when(z == 0)
    def _():
        ship_queries().start()

    mst[...] = jnp.full(mst.shape, NEG, F32)
    lst[...] = jnp.zeros(lst.shape, F32)
    acc[...] = jnp.zeros(acc.shape, F32)

    def attend(m, heads, groups):
        work = [(h, qp, keys) for h in heads for qp, keys in groups]
        scores = []
        for h, qp, keys in work:
            q = qbuf[qp, h]
            scores.append([dot(kvbuf[m, piece, h, 0].reshape(2 * HALF, D), q, ((1,), (0,))) for piece, _ in keys])
        for (h, qp, keys), group in zip(work, scores):
            group = [s * SCALE2 + jnp.concatenate([bias[b]] * GROUP, axis=1) for s, (_, b) in zip(group, keys)]
            m_old = mst[qp, h]
            m_new = m_old
            for s in group:
                m_new = jnp.maximum(m_new, jnp.max(s, axis=0, keepdims=True))
            alpha = jnp.exp2(m_old - m_new)
            total = lst[qp, h] * alpha
            out = acc[qp, h] * alpha
            for s, (piece, _) in zip(group, keys):
                p = jnp.exp2(s - m_new)
                total = total + jnp.sum(p, axis=0, keepdims=True)
                vals = kvbuf[m, piece, h, 1]
                out = out + dot(jnp.concatenate([vals[0], vals[1]], axis=1), p.astype(BF16), ((1,), (0,)))
            mst[qp, h] = m_new
            lst[qp, h] = total
            acc[qp, h] = out

    back = jnp.transpose(perm[...].astype(F32), (1, 0)).astype(BF16)
    perm_t[...] = back

    def finish(h):
        outs = []
        for part in (E, L):
            total = lst[part, h]
            out = (acc[part, h] / total).astype(BF16)
            log = mst[part, h] * LN2 + jnp.log(total)
            outs.append(out)
            logs[h, :, part * GROUP * HALF:(part + 1) * GROUP * HALF] = log
        for g in range(0, GROUP, 2):
            stack = []
            for i in (g, g + 1):
                cols = slice(i * HALF, (i + 1) * HALF)
                stack.append(jnp.concatenate([outs[0][:, cols], outs[1][:, cols]], axis=1))
            two = dot(perm_t[...], jnp.concatenate(stack, axis=0), ((1,), (1,))).astype(BF16)
            o_ref[h * GROUP + g] = two[:, 0:D]
            o_ref[h * GROUP + g + 1] = two[:, D:]

    def step(event):
        kind = event // 64
        m = (event // 8) % CHIPS
        low = event % 8

        @pl.when(kind == 0)
        def _():
            across(m, low).wait_recv()
            forward(m, low)

        for g, heads in enumerate(GROUPS):
            @pl.when(jnp.logical_and(kind == 1, low == g))
            def _():
                partner(m, g).wait_recv()

                @pl.when(m >= own)
                def _():
                    partner(m, 2 + g).wait_recv()

                away = z == 0 if g == 1 else z < 0
                here = jnp.logical_not(away)

                @pl.when(jnp.logical_and(here, m > own))
                def _():
                    attend(m, heads, [(L, [(E, 0), (L, 0)])])

                @pl.when(jnp.logical_and(here, m < own))
                def _():
                    attend(m, heads, [(E, [(E, 0)]), (L, [(E, 0)])])

                @pl.when(jnp.logical_and(here, m == own))
                def _():
                    attend(m, heads, [(E, [(E, 1)]), (L, [(L, 2), (E, 0)])])

                if g == 1:
                    @pl.when(away)
                    def _():
                        attend(m, heads, [(E, [(E, jnp.where(m == own, 1, 0))])])

        @pl.when(jnp.logical_and(kind == 2, jnp.logical_or(low == 0, low == 2)))
        def _():
            @pl.when(low == 2)
            def _():
                ship_queries().wait_recv()

            @pl.when(jnp.logical_and(m >= y, m < own))
            def _():
                partner(m, PARTS - 1).wait_recv()

            @pl.when(m >= y)
            def _():
                attend(m, GROUPS[1], [(GUEST, [(E, 0), (L, jnp.where(m == y, 2, 0))])])

            @pl.when(m < y)
            def _():
                attend(m, GROUPS[1], [(GUEST, [(E, 0)])])

        @pl.when(jnp.logical_and(kind == 2, low == 1))
        def _():
            total = lst[GUEST, KVH - 1]
            x_out[...] = (acc[GUEST, KVH - 1] / total).astype(BF16)
            x_log[...] = mst[GUEST, KVH - 1] * LN2 + jnp.log(total)
            for x in ship_results():
                x.start()

        @pl.when(jnp.logical_and(kind == 2, low == 4))
        def _():
            for h in GROUPS[0]:
                finish(h)

        @pl.when(jnp.logical_and(kind == 2, low == 5))
        def _():
            @pl.when(z == 0)
            def _():
                for x in ship_results():
                    x.wait_recv()
                acc[L, KVH - 1] = x_out[...].astype(F32)
                lst[L, KVH - 1] = jnp.ones((1, GROUP * HALF), F32)
                mst[L, KVH - 1] = x_log[...] * LOG2E

            finish(KVH - 1)

    @pl.loop(0, WORDS)
    def _(n):
        word = select(n, event_words)

        @pl.loop(0, PER_WORD)
        def _(i):
            step(jnp.right_shift(word, BITS * i) % (1 << BITS))

    lse = []
    for part in (E, L):
        rows = []
        for h in range(KVH):
            for g in range(GROUP):
                at = (part * GROUP + g) * HALF
                rows.append(logs[h, :, at:at + HALF])
        lse.append(jnp.concatenate(rows, axis=0))
    lse = jnp.concatenate(lse, axis=1)
    lse_ref[...] = dot(lse, perm[...].astype(F32), ((1,), (0,)), precision=lax.Precision.HIGHEST)

    for m in range(CHIPS):
        entry = jnp.right_shift(route_words[m // 2], 16 * (m % 2))
        for part in range(PARTS):
            for bit, way in ((3 * part, down), (3 * part + 1, across), (3 * part + 2, up), (3 * PARTS + part, partner)):
                pl.when(jnp.right_shift(entry, bit) % 2 == 1)(way(m, part).wait_send)

    @pl.when(z == 0)
    def _():
        ship_queries().wait_send()

    @pl.when(z == 1)
    def _():
        for x in ship_results():
            x.wait_send()


def solution(mesh):
    half = np.arange(D // 2, dtype=np.float32) * np.float32(2.0) / np.float32(D)
    freq = np.power(np.float64(THETA), -half.astype(np.float64)).astype(np.float32)
    freq = np.concatenate([freq, freq])[None, :]

    def per_device(q_raw, k_raw, v_raw, positions, seq_ids, q_gain, k_gain):
        vmem = pl.BlockSpec(memory_space=pltpu.VMEM)
        hbm = pl.BlockSpec(memory_space=pltpu.HBM)
        sem = pltpu.SemaphoreType.DMA((CHIPS, PARTS))
        inputs = (q_raw, k_raw, v_raw, positions[None, :], seq_ids[None, :], q_gain[None, :], k_gain[None, :], jnp.asarray(freq))
        out, lse = pl.pallas_call(
            kernel,
            out_shape=(jax.ShapeDtypeStruct((QH, T, D), BF16), jax.ShapeDtypeStruct((QH, T), F32)),
            in_specs=[hbm] * 8,
            out_specs=(vmem, vmem),
            scratch_shapes=[
                pltpu.VMEM((CHIPS, 2, KVH, 2, 2, HALF, D), BF16),
                pltpu.VMEM((3, KVH, D, GROUP * HALF), BF16),
                pltpu.VMEM((3, KVH, D, GROUP * HALF), F32),
                pltpu.VMEM((3, KVH, 1, GROUP * HALF), F32),
                pltpu.VMEM((3, KVH, 1, GROUP * HALF), F32),
                pltpu.VMEM((3, 2 * HALF, HALF), F32),
                pltpu.VMEM((2, T, D), F32),
                pltpu.VMEM((T, T), BF16),
                pltpu.VMEM((T, QH, D), BF16),
                pltpu.VMEM((T, KVH, D), BF16),
                pltpu.VMEM((T, KVH, D), BF16),
                pltpu.VMEM((1, T), jnp.int32),
                pltpu.VMEM((1, T), jnp.int32),
                pltpu.VMEM((1, D), BF16),
                pltpu.VMEM((1, D), BF16),
                pltpu.VMEM((1, D), F32),
                sem, sem, sem, sem, sem, sem,
                pltpu.SemaphoreType.DMA((8,)),
                pltpu.SemaphoreType.DMA((3,)),
                pltpu.SemaphoreType.DMA((3,)),
                pltpu.VMEM((T, T), BF16),
                pltpu.VMEM((KVH, 1, 2 * GROUP * HALF), F32),
                pltpu.VMEM((D, GROUP * HALF), BF16),
                pltpu.VMEM((1, GROUP * HALF), F32),
            ],
            compiler_params=pltpu.CompilerParams(collective_id=0, has_side_effects=True, vmem_limit_bytes=48 * 1024 * 1024),
            name="gather_attend",
        )(*[pltpu.with_memory_space_constraint(x, pltpu.HBM) for x in inputs])
        return jnp.transpose(out, (1, 0, 2)), lse.T

    return jax.shard_map(per_device, mesh=mesh, in_specs=(P("cp", "tp", None), P("cp", "tp", None), P("cp", "tp", None), P("cp"), P("cp"), P(), P()), out_specs=(P("cp", "tp", None), P("cp", "tp")), check_vma=False)
```

```python
import functools
import math

import jax
import jax.numpy as jnp
import numpy as np
from jax import lax
from jax.experimental import pallas as pl
from jax.experimental.pallas import tpu as pltpu
from jax.sharding import PartitionSpec as P

THETA = 1000000.0
EPS = 1e-6
NEG = -1e30
LAYERS = 4
CHIPS = 8
CP = 16
T = 256
HALF = 128
KVH = 4
GROUP = 4
QH = KVH * GROUP
D = 128
LOG2E = math.log2(math.e)
LN2 = math.log(2.0)
SCALE2 = D ** -0.5 * LOG2E
EVENTS = (
    (0x12084140, 0x0a501009, 0x18481a0b, 0x222a5820, 0x68322860, 0x3a703038, 0xff858478, 0xffffffff, 0xffffffff, 0xffffffff, 0xffffffff, 0xffffffff, 0xffffffff, 0xffffffff),
    (0x1a490148, 0x18400041, 0x102a1258, 0x38682850, 0x78223a20, 0x70303260, 0xffff8584, 0xffffffff, 0xffffffff, 0xffffffff, 0xffffffff, 0xffffffff, 0xffffffff, 0xffffffff),
    (0x231b0151, 0x00412150, 0x0320611a, 0x90821840, 0x58a01922, 0x59330831, 0x7198092a, 0x49b00b29, 0x48882b32, 0x3028a869, 0x38683b60, 0xb8797039, 0x7885813a, 0xffffff84),
    (0x10085859, 0x2911092a, 0x2b130b48, 0x23514901, 0x2128908a, 0x61804198, 0x003869a0, 0x3a4050a8, 0x393b6820, 0x31792278, 0x336030b8, 0x3281b071, 0xff847085, 0xffffffff),
    (0x10333160, 0x1150612a, 0x2b320129, 0x69514171, 0x68003028, 0x1838403b, 0x08581970, 0x09483a59, 0x79497839, 0xffff8584, 0xffffffff, 0xffffffff, 0xffffffff, 0xffffffff),
    (0x18692168, 0x19206138, 0x333a3158, 0x083b6059, 0x10097139, 0x49110148, 0x32504130, 0x00707851, 0x84408579, 0xffffffff, 0xffffffff, 0xffffffff, 0xffffffff, 0xffffffff),
    (0x38712170, 0x3a602061, 0x3978103b, 0x01295011, 0x79416951, 0x68190028, 0x58185940, 0x84094808, 0xffff8549, 0xffffffff, 0xffffffff, 0xffffffff, 0xffffffff, 0xffffffff),
    (0x79312978, 0x71302869, 0x70616821, 0x58192018, 0x11106059, 0x48095108, 0x00504901, 0x84408541, 0xffffffff, 0xffffffff, 0xffffffff, 0xffffffff, 0xffffffff, 0xffffffff),
)
ROUTES = (
    (0x5824f836, 0x50005082, 0x50005082, 0x50005080),
    (0xfcb63000, 0x50025000, 0x50825000, 0x50825000),
    (0xb024b036, 0xf044f477, 0xf000f4d3, 0xf000f4d1),
    (0xb0243020, 0xf4f7b000, 0xf4d3f000, 0xf0c3f001),
    (0x30243026, 0x30043036, 0xf000f27f, 0xf208f6d9),
    (0x30243020, 0x30343000, 0xf6ff3020, 0xf2dbf001),
    (0x30003002, 0x30003012, 0x30003002, 0xf200f25b),
    (0x30003000, 0x30103000, 0x30123000, 0xf6db3001),
)
FIRST = (0x60a, 0x688, 0x642, 0x213, 0x40b, 0x0ca, 0x099, 0x2d0)
GUEST = 2
BITS = 8
PER_WORD = 4
WORDS = len(EVENTS[0])
PARTS = 4
GROUPS = ((0, 1, 2), (3,))


def signed(word):
    return word - (1 << 32) if word >= 1 << 31 else word


def select(index, values):
    values = [jnp.int32(v) if isinstance(v, int) else v for v in values]
    while len(values) > 1:
        odd = index % 2 == 1
        values = [jnp.where(odd, values[i + 1], values[i]) if i + 1 < len(values) else values[i] for i in range(0, len(values), 2)]
        index = index // 2
    return values[0]


E, L = 0, 1
F32 = jnp.float32
BF16 = jnp.bfloat16
MESH = pl.DeviceIdType.MESH


def dot(a, b, dims, precision=None):
    return lax.dot_general(a, b, (dims, ((), ())), preferred_element_type=F32, precision=precision)


def column(row, ident):
    return jnp.sum(jnp.where(ident, row, 0.0), axis=1, keepdims=True)


def norm_rope(x, gain, cos, sin):
    inv = lax.rsqrt(jnp.mean(x * x, axis=-1, keepdims=True) + EPS)
    normed = (x * inv * gain).astype(BF16).astype(F32)
    return (normed * cos + pltpu.roll(normed, D // 2, 1) * sin).astype(BF16)


def kernel(q_hbm, k_hbm, v_hbm, pos_hbm, seq_hbm, qg_hbm, kg_hbm, freq_hbm, o_ref, lse_ref,
           kvbuf, qbuf, acc, mst, lst, bias, rope, perm,
           q_in, k_in, v_in, pos_ref, seq_ref, qg_ref, kg_ref, freq_ref,
           s_dn, s_up, s_y, s_d, r_link, r_d, s_in, s_x, r_x,
           perm_t, logs, x_out, x_log):
    me = lax.axis_index("cp")
    z = me // 4
    y = (me // 2) % 2
    c = me % 2
    own = me // 2

    def dev(zz, yy, cc):
        return {"cp": zz * 4 + yy * 2 + cc}

    barrier = pltpu.get_barrier_semaphore()
    pl.semaphore_signal(barrier, inc=1, device_id=dev(z, y, 1 - c), device_id_type=MESH)
    pl.semaphore_signal(barrier, inc=1, device_id=dev(z, 1 - y, c), device_id_type=MESH)

    @pl.when(z > 0)
    def _():
        pl.semaphore_signal(barrier, inc=1, device_id=dev(z - 1, y, c), device_id_type=MESH)

    @pl.when(z < LAYERS - 1)
    def _():
        pl.semaphore_signal(barrier, inc=1, device_id=dev(z + 1, y, c), device_id_type=MESH)

    pairs = ((pos_hbm, pos_ref), (seq_hbm, seq_ref), (freq_hbm, freq_ref), (kg_hbm, kg_ref), (k_hbm, k_in), (v_hbm, v_in),
             (qg_hbm, qg_ref), (q_hbm, q_in))
    loads = [pltpu.make_async_copy(src, dst, s_in.at[i]) for i, (src, dst) in enumerate(pairs)]
    for load in loads:
        load.start()
    loads[0].wait()
    loads[1].wait()

    row_i = lax.broadcasted_iota(jnp.int32, (T, T), 0)
    col_i = lax.broadcasted_iota(jnp.int32, (T, T), 1)
    ident = row_i == col_i
    pos_row = pos_ref[...].astype(F32)
    seq_row = seq_ref[...].astype(F32)
    pos_col = column(pos_row, ident)
    seq_col = column(seq_row, ident)
    same = (seq_col == seq_row).astype(F32)
    early_row = (pos_row < 8.0 * jnp.sum(same, axis=0, keepdims=True)).astype(F32)
    early_col = (pos_col < 8.0 * jnp.sum(same, axis=1, keepdims=True)).astype(F32)
    alike = (early_col == early_row).astype(F32)
    dest_row = jnp.sum(jnp.where(row_i < col_i, alike, 0.0), axis=0, keepdims=True) + HALF * (1.0 - early_row)
    one_hot = (row_i.astype(F32) == dest_row).astype(BF16)
    perm[...] = one_hot

    left = lax.broadcasted_iota(jnp.int32, (HALF, D), 1) < D // 2
    loads[2].wait()
    angle = jnp.where(left, pos_col[:HALF], pos_col[HALF:]) * freq_ref[...]
    cos = jnp.cos(angle)
    sin = jnp.sin(angle)
    cos_r = pltpu.roll(cos, D // 2, 1)
    sin_r = pltpu.roll(sin, D // 2, 1)
    cos = jnp.concatenate([jnp.where(left, cos, cos_r), jnp.where(left, cos_r, cos)], axis=0)
    sin = jnp.concatenate([jnp.where(left, -sin, sin_r), jnp.where(left, -sin_r, sin)], axis=0)
    rope[0] = cos
    rope[1] = sin

    loads[3].wait()
    loads[4].wait()
    loads[5].wait()
    k_all = jnp.transpose(k_in[...].astype(F32), (1, 0, 2))
    v_all = jnp.transpose(v_in[...].astype(F32), (1, 0, 2)).astype(BF16)
    gain = kg_ref[...].astype(F32)
    for h in range(KVH):
        kr = dot(one_hot, norm_rope(k_all[h], gain, cos, sin), ((1,), (0,))).astype(BF16)
        vr = dot(v_all[h], one_hot, ((0,), (1,))).astype(BF16)
        for part in (E, L):
            kvbuf[own, part, h, 0, c] = kr[part * HALF:(part + 1) * HALF]
            kvbuf[own, part, h, 1, c] = vr[:, part * HALF:(part + 1) * HALF]

    pl.semaphore_wait(barrier, 2 + jnp.minimum(z, 1) + jnp.minimum(LAYERS - 1 - z, 1))

    class Copy:
        def __init__(self, m, part, send, recv, target):
            self.args = (m, part, send, recv, target)

        def act(self, name):
            m, part, send, recv, target = self.args

            def run(g):
                ref = kvbuf.at[m, part // 2, pl.ds(GROUPS[g][0], len(GROUPS[g])), :, c]
                getattr(pltpu.make_async_remote_copy(
                    src_ref=ref, dst_ref=ref, send_sem=send.at[m, part], recv_sem=recv.at[m, part],
                    device_id=target, device_id_type=MESH), name)()

            if isinstance(part, int):
                run(part % 2)
            else:
                pl.when(part % 2 == 0)(lambda: run(0))
                pl.when(part % 2 == 1)(lambda: run(1))

        def start(self):
            self.act("start")

        def wait_recv(self):
            self.act("wait_recv")

        def wait_send(self):
            self.act("wait_send")

    def down(m, part):
        return Copy(m, part, s_dn, r_link, dev(z - 1, y, c))

    def up(m, part):
        return Copy(m, part, s_up, r_link, dev(z + 1, y, c))

    def across(m, part):
        return Copy(m, part, s_y, r_link, dev(z, 1 - y, c))

    def partner(m, part):
        return Copy(m, part, s_d, r_d, dev(z, y, 1 - c))

    route_words = [select(own, [signed(row[pair]) for row in ROUTES]) for pair in range(CHIPS // 2)]
    first_word = select(own, list(FIRST))

    def routes(m, part):
        entry = jnp.right_shift(select(m // 2, route_words), 16 * (m % 2))
        way = jnp.right_shift(entry, 3 * part) % 8
        need = jnp.right_shift(entry, 3 * PARTS + part) % 2
        return way % 2 == 1, (way // 2) % 2 == 1, way // 4 == 1, need == 1

    def forward(m, part):
        go_down, go_across, go_up, go_partner = routes(m, part)

        @pl.when(go_down)
        def _():
            down(m, part).start()

        @pl.when(go_across)
        def _():
            across(m, part).start()

        @pl.when(go_up)
        def _():
            up(m, part).start()

        @pl.when(go_partner)
        def _():
            partner(m, part).start()

    @pl.loop(0, PARTS)
    def _(i):
        forward(own, jnp.right_shift(first_word, 3 * i) % 8)

    event_words = [select(own, [signed(row[w]) for row in EVENTS]) for w in range(WORDS)]

    loads[6].wait()
    loads[7].wait()
    q_all = jnp.transpose(q_in[...].astype(F32), (1, 0, 2))
    q_gain = qg_ref[...].astype(F32)
    for h in range(QH):
        qr = dot(norm_rope(q_all[h], q_gain, rope[0], rope[1]), perm[...], ((0,), (1,))).astype(BF16)
        for part in (E, L):
            qbuf[part, h // GROUP, :, (h % GROUP) * HALF:(h % GROUP + 1) * HALF] = qr[:, part * HALF:(part + 1) * HALF]

    def ship(i, src, dst, zz):
        return pltpu.make_async_remote_copy(
            src_ref=src, dst_ref=dst, send_sem=s_x.at[i], recv_sem=r_x.at[i], device_id=dev(zz, y, c), device_id_type=MESH)

    def ship_queries():
        return ship(0, qbuf.at[L, KVH - 1], qbuf.at[GUEST, KVH - 1], 1 - z)

    def ship_results():
        return ship(1, x_out, x_out, 1 - z), ship(2, x_log, x_log, 1 - z)

    seg = dot(perm[0:HALF], same.astype(BF16), ((1,), (0,))).astype(BF16)
    seg = dot(seg, perm[0:HALF], ((1,), (1,))) > 0.5
    r_i = lax.broadcasted_iota(jnp.int32, (HALF, HALF), 0)
    c_i = lax.broadcasted_iota(jnp.int32, (HALF, HALF), 1)
    full = jnp.where(seg, 0.0, NEG)
    diag = jnp.where(jnp.logical_and(seg, r_i <= c_i), 0.0, NEG)
    none = jnp.full((HALF, HALF), NEG, F32)
    first = c == 0
    bias[0, 0:HALF] = full
    bias[0, HALF:] = full
    bias[1, 0:HALF] = jnp.where(first, diag, full)
    bias[1, HALF:] = jnp.where(first, none, diag)
    bias[2, 0:HALF] = jnp.where(first, diag, none)
    bias[2, HALF:] = jnp.where(first, full, diag)

    @pl.when(z == 0)
    def _():
        ship_queries().start()

    mst[...] = jnp.full(mst.shape, NEG, F32)
    lst[...] = jnp.zeros(lst.shape, F32)
    acc[...] = jnp.zeros(acc.shape, F32)

    def attend(m, heads, groups):
        work = [(h, qp, keys) for h in heads for qp, keys in groups]
        scores = []
        for h, qp, keys in work:
            q = qbuf[qp, h]
            scores.append([dot(kvbuf[m, piece, h, 0].reshape(2 * HALF, D), q, ((1,), (0,))) for piece, _ in keys])
        for (h, qp, keys), group in zip(work, scores):
            group = [s * SCALE2 + jnp.concatenate([bias[b]] * GROUP, axis=1) for s, (_, b) in zip(group, keys)]
            m_old = mst[qp, h]
            m_new = m_old
            for s in group:
                m_new = jnp.maximum(m_new, jnp.max(s, axis=0, keepdims=True))
            alpha = jnp.exp2(m_old - m_new)
            total = lst[qp, h] * alpha
            out = acc[qp, h] * alpha
            for s, (piece, _) in zip(group, keys):
                p = jnp.exp2(s - m_new)
                total = total + jnp.sum(p, axis=0, keepdims=True)
                vals = kvbuf[m, piece, h, 1]
                out = out + dot(jnp.concatenate([vals[0], vals[1]], axis=1), p.astype(BF16), ((1,), (0,)))
            mst[qp, h] = m_new
            lst[qp, h] = total
            acc[qp, h] = out

    back = jnp.transpose(perm[...].astype(F32), (1, 0)).astype(BF16)
    perm_t[...] = back

    def finish(h):
        outs = []
        for part in (E, L):
            total = lst[part, h]
            out = (acc[part, h] / total).astype(BF16)
            log = mst[part, h] * LN2 + jnp.log(total)
            outs.append(out)
            logs[h, :, part * GROUP * HALF:(part + 1) * GROUP * HALF] = log
        for g in range(0, GROUP, 2):
            stack = []
            for i in (g, g + 1):
                cols = slice(i * HALF, (i + 1) * HALF)
                stack.append(jnp.concatenate([outs[0][:, cols], outs[1][:, cols]], axis=1))
            two = dot(perm_t[...], jnp.concatenate(stack, axis=0), ((1,), (1,))).astype(BF16)
            o_ref[h * GROUP + g] = two[:, 0:D]
            o_ref[h * GROUP + g + 1] = two[:, D:]

    def step(event):
        kind = event // 64
        m = (event // 8) % CHIPS
        low = event % 8

        @pl.when(kind == 0)
        def _():
            across(m, low).wait_recv()
            forward(m, low)

        for g, heads in enumerate(GROUPS):
            @pl.when(jnp.logical_and(kind == 1, low == g))
            def _():
                partner(m, g).wait_recv()

                @pl.when(m >= own)
                def _():
                    partner(m, 2 + g).wait_recv()

                away = z == 0 if g == 1 else z < 0
                here = jnp.logical_not(away)

                @pl.when(jnp.logical_and(here, m > own))
                def _():
                    attend(m, heads, [(L, [(E, 0), (L, 0)])])

                @pl.when(jnp.logical_and(here, m < own))
                def _():
                    attend(m, heads, [(E, [(E, 0)]), (L, [(E, 0)])])

                @pl.when(jnp.logical_and(here, m == own))
                def _():
                    attend(m, heads, [(E, [(E, 1)]), (L, [(L, 2), (E, 0)])])

                if g == 1:
                    @pl.when(away)
                    def _():
                        attend(m, heads, [(E, [(E, jnp.where(m == own, 1, 0))])])

        @pl.when(jnp.logical_and(kind == 2, jnp.logical_or(low == 0, low == 2)))
        def _():
            @pl.when(low == 2)
            def _():
                ship_queries().wait_recv()

            @pl.when(jnp.logical_and(m >= y, m < own))
            def _():
                partner(m, PARTS - 1).wait_recv()

            @pl.when(m >= y)
            def _():
                attend(m, GROUPS[1], [(GUEST, [(E, 0), (L, jnp.where(m == y, 2, 0))])])

            @pl.when(m < y)
            def _():
                attend(m, GROUPS[1], [(GUEST, [(E, 0)])])

        @pl.when(jnp.logical_and(kind == 2, low == 1))
        def _():
            total = lst[GUEST, KVH - 1]
            x_out[...] = (acc[GUEST, KVH - 1] / total).astype(BF16)
            x_log[...] = mst[GUEST, KVH - 1] * LN2 + jnp.log(total)
            for x in ship_results():
                x.start()

        @pl.when(jnp.logical_and(kind == 2, low == 4))
        def _():
            for h in GROUPS[0]:
                finish(h)

        @pl.when(jnp.logical_and(kind == 2, low == 5))
        def _():
            @pl.when(z == 0)
            def _():
                for x in ship_results():
                    x.wait_recv()
                acc[L, KVH - 1] = x_out[...].astype(F32)
                lst[L, KVH - 1] = jnp.ones((1, GROUP * HALF), F32)
                mst[L, KVH - 1] = x_log[...] * LOG2E

            finish(KVH - 1)

    @pl.loop(0, WORDS)
    def _(n):
        word = select(n, event_words)

        @pl.loop(0, PER_WORD)
        def _(i):
            step(jnp.right_shift(word, BITS * i) % (1 << BITS))

    lse = []
    for part in (E, L):
        rows = []
        for h in range(KVH):
            for g in range(GROUP):
                at = (part * GROUP + g) * HALF
                rows.append(logs[h, :, at:at + HALF])
        lse.append(jnp.concatenate(rows, axis=0))
    lse = jnp.concatenate(lse, axis=1)
    lse_ref[...] = dot(lse, perm[...].astype(F32), ((1,), (0,)), precision=lax.Precision.HIGHEST)

    for m in range(CHIPS):
        entry = jnp.right_shift(route_words[m // 2], 16 * (m % 2))
        for part in range(PARTS):
            for bit, way in ((3 * part, down), (3 * part + 1, across), (3 * part + 2, up), (3 * PARTS + part, partner)):
                pl.when(jnp.right_shift(entry, bit) % 2 == 1)(way(m, part).wait_send)

    @pl.when(z == 0)
    def _():
        ship_queries().wait_send()

    @pl.when(z == 1)
    def _():
        for x in ship_results():
            x.wait_send()


def solution(mesh):
    half = np.arange(D // 2, dtype=np.float32) * np.float32(2.0) / np.float32(D)
    freq = np.power(np.float64(THETA), -half.astype(np.float64)).astype(np.float32)
    freq = np.concatenate([freq, freq])[None, :]

    def per_device(q_raw, k_raw, v_raw, positions, seq_ids, q_gain, k_gain):
        vmem = pl.BlockSpec(memory_space=pltpu.VMEM)
        hbm = pl.BlockSpec(memory_space=pltpu.HBM)
        sem = pltpu.SemaphoreType.DMA((CHIPS, PARTS))
        inputs = (q_raw, k_raw, v_raw, positions[None, :], seq_ids[None, :], q_gain[None, :], k_gain[None, :], jnp.asarray(freq))
        out, lse = pl.pallas_call(
            kernel,
            out_shape=(jax.ShapeDtypeStruct((QH, T, D), BF16), jax.ShapeDtypeStruct((QH, T), F32)),
            in_specs=[hbm] * 8,
            out_specs=(vmem, vmem),
            scratch_shapes=[
                pltpu.VMEM((CHIPS, 2, KVH, 2, 2, HALF, D), BF16),
                pltpu.VMEM((3, KVH, D, GROUP * HALF), BF16),
                pltpu.VMEM((3, KVH, D, GROUP * HALF), F32),
                pltpu.VMEM((3, KVH, 1, GROUP * HALF), F32),
                pltpu.VMEM((3, KVH, 1, GROUP * HALF), F32),
                pltpu.VMEM((3, 2 * HALF, HALF), F32),
                pltpu.VMEM((2, T, D), F32),
                pltpu.VMEM((T, T), BF16),
                pltpu.VMEM((T, QH, D), BF16),
                pltpu.VMEM((T, KVH, D), BF16),
                pltpu.VMEM((T, KVH, D), BF16),
                pltpu.VMEM((1, T), jnp.int32),
                pltpu.VMEM((1, T), jnp.int32),
                pltpu.VMEM((1, D), BF16),
                pltpu.VMEM((1, D), BF16),
                pltpu.VMEM((1, D), F32),
                sem, sem, sem, sem, sem, sem,
                pltpu.SemaphoreType.DMA((8,)),
                pltpu.SemaphoreType.DMA((3,)),
                pltpu.SemaphoreType.DMA((3,)),
                pltpu.VMEM((T, T), BF16),
                pltpu.VMEM((KVH, 1, 2 * GROUP * HALF), F32),
                pltpu.VMEM((D, GROUP * HALF), BF16),
                pltpu.VMEM((1, GROUP * HALF), F32),
            ],
            compiler_params=pltpu.CompilerParams(collective_id=0, has_side_effects=True, vmem_limit_bytes=48 * 1024 * 1024),
            name="gather_attend",
        )(*[pltpu.with_memory_space_constraint(x, pltpu.HBM) for x in inputs])
        return jnp.transpose(out, (1, 0, 2)), lse.T

    return jax.shard_map(per_device, mesh=mesh, in_specs=(P("cp", "tp", None), P("cp", "tp", None), P("cp", "tp", None), P("cp"), P("cp"), P(), P()), out_specs=(P("cp", "tp", None), P("cp", "tp")), check_vma=False)
```
